256 devices in a mesh: groups: 2 (over y), seq: 8 (over x, core), tensor: 16 (over z).
Axes of the slice: x: 4, y: 2, z: 16, core: 2. Of those that a mesh axis runs over, the one named last changes fastest.
The devices are a block of a 4x16x16 slice.
Arguments:
- hidden: bfloat16 [512, 4608], P(('groups', 'seq')), parts along dimension 0, may hold values from -6 to 6
- pre_gain: float32 [4608], replicated, may hold values from 0.25 to 1.75
- w_query: bfloat16 [4608, 4096], P(None, 'tensor'), may hold values from -0.09375 to 0.09375
- w_key: bfloat16 [4608, 2048], P(None, 'tensor'), may hold values from -0.09375 to 0.09375
- w_value: bfloat16 [4608, 2048], P(None, 'tensor'), may hold values from -0.09375 to 0.09375
- w_out: bfloat16 [4096, 4608], P('tensor'), may hold values from -0.125 to 0.125
- post_gain: float32 [4608], P('tensor'), may hold values from 0.25 to 1.75
- cache_pool: bfloat16 [1024, 2, 128, 2048], P(('groups', 'seq'), None, None, 'tensor'), parts along dimension 0, may hold values from -6 to 6
- prompt_cache: bfloat16 [256, 2, 64, 2048], P('seq', None, None, 'tensor'), may hold values from -6 to 6
- task_ids: int32 [512], P('groups'), parts along dimension 0, may hold values from 0 to 255
- cache_lengths: int32 [512], P('groups'), parts along dimension 0, may hold values from 1 to 4096, as said below
- block_table: int32 [512, 32], P('groups'), parts along dimension 0, may hold values from -1 to 511, as said below
Outputs:
- layer_out: bfloat16 [512, 4608], P(('groups', 'seq'), 'tensor'), parts along dimension 0
- fresh_cache: bfloat16 [512, 2, 2048], P(('groups', 'seq'), None, 'tensor'), parts along dimension 0
The draws below stay inside these ranges and needn't reach their ends.
There are 2 independent parts, one for each index of `groups`. The reference program is written for one: setup_inputs(seed, part) draws one part's arguments, and reference() takes and returns one part's arrays. A program takes and returns all parts, laid end to end along the dimension named above; an argument that names none is the same for every part. Nothing has to cross between parts.
Inputs may be any that keep to these rules, and one draw needn't show every extreme that they name: `cache_lengths`: each draw has a request with exactly 4096 cache tokens. block_table[r, j] is the page of cache_pool holding cache tokens j * 128 to (j + 1) * 128 - 1 of request r for j < ceil(cache_lengths[r] / 128), and -1 for the later j; no page is named twice.
All inputs are finite; a program needn't handle non-finite values.
Results may differ from the reference program's by a relative error of at most 0.018.
Values may be sent and summed in bfloat16 or wider, within the bound.
A program may use at most 64 MiB of HBM per device.

```python
import math
import jax
import jax.numpy as jnp
import numpy as np
from jax import lax

D = 4608
H = 32
KVH = 16
HD = 128
BLOCK = 128
PROMPT = 64
MAXLEN = 4096
MAXBLK = 32
TASKS = 256
REQ = 256
POOL = 512


def lengths_and_blocks(key):
    base = jax.random.fold_in(key, 7)
    k_first, k_second, k_order, k_tail, k_large, k_pages = jax.random.split(base, 6)
    extra = POOL - REQ - MAXBLK
    first_pick = jax.random.randint(k_first, (extra,), 0, REQ)
    second_pick = jax.random.randint(k_second, (extra,), 0, REQ)
    skewed = first_pick * second_pick // REQ
    order = jax.random.permutation(k_order, REQ)
    picked = order[skewed]
    counts = jnp.sum((picked[:, None] == jnp.arange(REQ)[None, :]).astype(jnp.int32), axis=0)
    largest = jax.random.randint(k_large, (), 0, REQ)
    is_large = jnp.arange(REQ) == largest
    blocks = jnp.where(is_large, MAXBLK, jnp.minimum(1 + counts, MAXBLK)).astype(jnp.int32)
    tails = jax.random.randint(k_tail, (REQ,), 1, BLOCK + 1)
    lengths = jnp.where(is_large, MAXLEN, (blocks - 1) * BLOCK + tails)
    offsets = jnp.cumsum(blocks) - blocks
    pages = jax.random.permutation(k_pages, POOL)
    slots = offsets[:, None] + jnp.arange(MAXBLK)[None, :]
    live_slot = jnp.arange(MAXBLK)[None, :] < blocks[:, None]
    table = jnp.where(live_slot, pages[jnp.minimum(slots, POOL - 1)], -1)
    return (lengths.astype(jnp.int32), table.astype(jnp.int32))


def draw_cache_lengths(key, part):
    return lengths_and_blocks(key)[0]


def draw_block_table(key, part):
    return lengths_and_blocks(key)[1]


def place_ends(values, own_key, least, high):
    longest = values.shape.index(max(values.shape))
    spots = []
    for shift in (0, 1):
        where = [jax.random.randint(jax.random.fold_in(own_key, axis), (), 0, length) for axis, length in enumerate(values.shape)]
        where[longest] = (where[longest] + shift) % values.shape[longest]
        spots.append(tuple(where))
    return values.at[spots[0]].set(least).at[spots[1]].set(high)


def spiked(drawn, stream_key, source, target, shards_of, factor):
    owner, partner = [(jnp.arange(drawn.shape[dim]) // (drawn.shape[dim] // shards_of)).reshape([-1 if axis == dim else 1 for axis in range(drawn.ndim)]) for dim in (source, target)]
    chosen = jax.random.permutation(stream_key, shards_of)[partner]
    strong = (owner == chosen) | (owner == (partner + shards_of // 2) % shards_of)
    return jnp.where(strong, factor * drawn, drawn)


def shard_levels(own_key, dims, pieces, low, high):
    loudness = 1.0
    for dim, shards_of in pieces:
        draws = jax.random.uniform(jax.random.fold_in(jax.random.fold_in(own_key, 6), dim), (shards_of,), jnp.float32, low / len(pieces), high / len(pieces))
        loudness = loudness * jnp.repeat(jnp.exp(draws), dims[dim] // shards_of).reshape((-1,) + (1,) * (len(dims) - 1 - dim))
    return loudness


def cumulative_ranks(amount, skew):
    portions = [(1 << 20) // math.isqrt(rank ** skew) + 1 for rank in range(1, amount + 1)]
    spread = 1 + sum(portions) // (1 << 30)
    return np.cumsum(np.array([max(1, weight // spread) for weight in portions]))


def skewed_ids(stream_key, dims, count, lean):
    grid = cumulative_ranks(count, lean)
    ticket = jax.random.randint(jax.random.fold_in(stream_key, 1), dims, 0, int(grid[count - 1]))
    grade = jnp.searchsorted(jnp.asarray(grid, jnp.int32), ticket, side="right")
    return jax.random.permutation(jax.random.fold_in(stream_key, 2), count)[grade].astype(jnp.int32)


def bell_draw(key, extent, scale, most, cuts=(), kind=jnp.bfloat16):
    level = shard_levels(key, extent, cuts, -0.22, 0.18) if cuts else 1.0
    values = jax.random.normal(key, extent, jnp.float32) * scale * level
    return jnp.minimum(jnp.maximum(values, -most), most).astype(kind)


def heavy_noise(stream_key, extent, spread, bound, pieces, heavy, kind=jnp.bfloat16):
    array = spread * jax.random.normal(stream_key, extent, jnp.float32)
    if pieces:
        array = array * shard_levels(stream_key, extent, pieces, -0.22, 0.18)
    return jnp.clip(spiked(array, jax.random.fold_in(stream_key, 3), *heavy), -bound, bound).astype(kind)


def setup_inputs(seed: int = 0, part: int = 0) -> dict:
    key_list = jax.random.split(jax.random.key(seed), 13)
    part_keys = jax.random.split(jax.random.fold_in(key_list[12], part), 13)
    hidden = bell_draw(part_keys[0], (REQ, D), 1.0, 6.0, ((0, 8),))
    pre_gain = jnp.clip(1.0 + 0.15 * jax.random.normal(key_list[1], (D,), jnp.float32), 0.25, 1.75)
    w_query = bell_draw(key_list[2], (D, H * HD), D ** -0.5, 0.09375, ((1, 16),))
    w_key = bell_draw(key_list[3], (D, KVH * HD), D ** -0.5, 0.09375, ((1, 16),))
    w_value = bell_draw(key_list[4], (D, KVH * HD), D ** -0.5, 0.09375, ((1, 16),))
    w_out = heavy_noise(key_list[5], (H * HD, D), (H * HD) ** -0.5, 0.125, ((0, 16),), (0, 1, 16, 2.0))
    post_gain = jnp.clip(1.0 + 0.15 * jax.random.normal(key_list[6], (D,), jnp.float32), 0.25, 1.75)
    cache_pool = bell_draw(part_keys[7], (POOL, 2, BLOCK, KVH * HD), 1.0, 6.0, ((0, 8), (3, 16)))
    prompt_cache = bell_draw(key_list[8], (TASKS, 2, PROMPT, KVH * HD), 1.0, 6.0, ((0, 8), (3, 16)))
    task_ids = place_ends(skewed_ids(part_keys[9], (REQ,), TASKS, 2), jax.random.fold_in(part_keys[9], 3), 0, TASKS - 1).astype(jnp.int32)
    cache_lengths = draw_cache_lengths(jax.random.fold_in(jax.random.fold_in(key_list[12], part), 71), part)
    block_table = draw_block_table(jax.random.fold_in(jax.random.fold_in(key_list[12], part), 71), part)
    return dict(hidden=hidden, pre_gain=pre_gain, w_query=w_query, w_key=w_key, w_value=w_value, w_out=w_out, post_gain=post_gain, cache_pool=cache_pool, prompt_cache=prompt_cache, task_ids=task_ids, cache_lengths=cache_lengths, block_table=block_table)


cap_limit = 50.0

def rms_scale(values, gain):
    mean_square = lax.optimization_barrier(jnp.mean(values * values, axis=-1, keepdims=True))
    return values * lax.rsqrt(mean_square + 1e-06) * gain

def rotate(values, position):
    half_dim = values.shape[-1] // 2
    frequency = 10000.0 ** (-jnp.arange(half_dim, dtype=jnp.float32) / half_dim)
    angles = position.astype(jnp.float32)[:, None] * frequency[None, :]
    cosine = jnp.cos(angles)[:, None, :]
    sines = jnp.sin(angles)[:, None, :]
    first_half = values[..., :half_dim]
    second_half = values[..., half_dim:]
    return jnp.concatenate([first_half * cosine - second_half * sines, second_half * cosine + first_half * sines], axis=-1)

def capped(raw_score, score_scale):
    return cap_limit * jnp.tanh(raw_score * score_scale / cap_limit)

def reference(hidden, pre_gain, w_query, w_key, w_value, w_out, post_gain, cache_pool, prompt_cache, task_ids, cache_lengths, block_table):
    normed = rms_scale(hidden.astype(jnp.float32), pre_gain.astype(jnp.float32)).astype(jnp.bfloat16)
    position = (PROMPT + cache_lengths).astype(jnp.int32)
    query_rows = rotate(jnp.dot(normed, w_query, preferred_element_type=jnp.float32).reshape(REQ, H, HD), position).astype(jnp.bfloat16)
    key_new = rotate(jnp.dot(normed, w_key, preferred_element_type=jnp.float32).reshape(REQ, KVH, HD), position).astype(jnp.bfloat16)
    value_new = jnp.dot(normed, w_value, preferred_element_type=jnp.float32).astype(jnp.bfloat16)
    fresh_cache = jnp.stack([key_new.reshape(REQ, KVH * HD), value_new], axis=1)
    score_scale = float(D // H) ** (-0.5)
    group_size = H // KVH

    def one_request(request_args):
        query_one, task_one, length_one, row_one, key_one, value_one = request_args
        request_pages = cache_pool[jnp.maximum(row_one, 0)]
        cache_keys = request_pages[:, 0].reshape(MAXBLK * BLOCK, KVH, HD)
        cache_values = request_pages[:, 1].reshape(MAXBLK * BLOCK, KVH, HD)
        prompt = prompt_cache[task_one]
        all_keys = jnp.concatenate([prompt[0].reshape(PROMPT, KVH, HD), cache_keys, key_one[None]], axis=0)
        all_values = jnp.concatenate([prompt[1].reshape(PROMPT, KVH, HD), cache_values, value_one.reshape(1, KVH, HD)], axis=0)
        key_mask = jnp.concatenate([jnp.ones((PROMPT,), bool), jnp.arange(MAXBLK * BLOCK) < length_one, jnp.ones((1,), bool)])
        grouped = query_one.reshape(KVH, group_size, HD).astype(jnp.float32)
        raw_score = jnp.einsum('kgd,tkd->kgt', grouped, all_keys.astype(jnp.float32))
        weight = jnp.where(key_mask[None, None, :], jnp.exp(capped(raw_score, score_scale)), 0.0)
        weight_sum = lax.optimization_barrier(jnp.sum(weight, axis=-1))
        rounded = lax.optimization_barrier(weight.astype(jnp.bfloat16)).astype(jnp.float32)
        mixture = jnp.einsum('kgt,tkd->kgd', rounded, all_values.astype(jnp.float32))
        return (mixture / weight_sum[..., None]).reshape(H * HD).astype(jnp.bfloat16)
    attended = lax.map(one_request, (query_rows, task_ids, cache_lengths, block_table, key_new, value_new))
    projected = jnp.dot(attended, w_out, preferred_element_type=jnp.float32)
    layer_out = hidden.astype(jnp.float32) + rms_scale(projected, post_gain.astype(jnp.float32))
    return (layer_out.astype(jnp.bfloat16), fresh_cache)
```

```python
import functools
import math

import jax
import jax.numpy as jnp
import numpy as np
from jax import lax
from jax.experimental import pallas as pl
from jax.experimental.pallas import tpu as pltpu
from jax.sharding import PartitionSpec as P

D = 4608
H = 32
HD = 128
CAP = 50.0
EPS = 1e-6
MESH = pl.DeviceIdType.MESH
F32 = jnp.float32
BF16 = jnp.bfloat16
NT = (((1,), (1,)), ((), ()))
NN = (((1,), (0,)), ((), ()))

INNER = float(D // H) ** (-0.5) / CAP
OUTER = CAP * math.log2(math.e)


def dot(a, b, dims=NN):
    return lax.dot_general(a, b, dims, preferred_element_type=F32)


def weigh(raw):
    return jnp.exp2(OUTER * jnp.tanh(raw * INNER))


def iota(shape, dim):
    return lax.broadcasted_iota(jnp.int32, shape, dim)


def farthest_first(size):
    return sorted(range(1, size), key=lambda d: -min(d, size - d))


def layer(
    hidden_hbm,
    gain_hbm,
    wq_hbm,
    wk_hbm,
    wv_hbm,
    wo_hbm,
    post_hbm,
    pool_hbm,
    prompt_hbm,
    task_hbm,
    length_hbm,
    table_hbm,
    freq_hbm,
    out_ref,
    fresh_ref,
    hidden_v,
    gain_v,
    wq_v,
    wk_v,
    wv_v,
    wo_v,
    post_v,
    pool_v,
    prompt_v,
    task_v,
    length_v,
    table_v,
    freq_v,
    page_mix,
    all_query,
    mix_send,
    mix_recv,
    proj_send,
    proj_recv,
    square,
    in_sem,
    w_sem,
    q_send_sem,
    q_recv_sem,
    m_send_sem,
    m_recv_sem,
    p_send_sem,
    p_recv_sem,
    s_send_sem,
    s_recv_sem,
    *,
    seq,
    tensor,
    pieces,
):
    me = lax.axis_index("seq")
    mine = lax.axis_index("tensor")
    rows, width = hidden_v.shape
    requests = task_v.shape[1]
    pages = pool_v.shape[0]
    block = pool_v.shape[2]
    tasks, _, prompt, _ = prompt_v.shape
    blocks = table_v.shape[1]
    cols = out_ref.shape[1]

    seq_peer = lambda d: lax.rem(me + d, seq)
    seq_from = lambda d: lax.rem(me + seq - d, seq)
    tensor_peer = lambda d: lax.rem(mine + d, tensor)

    barrier = pltpu.get_barrier_semaphore()
    for d in range(1, seq):
        pl.semaphore_signal(barrier, inc=1, device_id={"seq": seq_peer(d)}, device_id_type=MESH)
    for d in range(1, tensor):
        pl.semaphore_signal(
            barrier, inc=1, device_id={"tensor": tensor_peer(d)}, device_id_type=MESH
        )

    small = [
        pltpu.make_async_copy(src, dst, in_sem.at[i])
        for i, (src, dst) in enumerate(
            (
                (hidden_hbm, hidden_v),
                (gain_hbm, gain_v),
                (length_hbm, length_v),
                (freq_hbm, freq_v),
                (table_hbm, table_v),
                (task_hbm, task_v),
                (post_hbm, post_v),
            )
        )
    ]
    for copy in small:
        copy.start()
    depth = width // pieces
    weights = []
    for i in range(pieces):
        part = pl.ds(i * depth, depth)
        weights.append(
            [
                pltpu.make_async_copy(src.at[part], dst.at[part], w_sem.at[3 * i + j])
                for j, (src, dst) in enumerate(
                    ((wq_hbm, wq_v), (wk_hbm, wk_v), (wv_hbm, wv_v))
                )
            ]
        )
    for group in weights:
        for copy in group:
            copy.start()
    bulk = [
        pltpu.make_async_copy(src, dst, in_sem.at[len(small) + i])
        for i, (src, dst) in enumerate(
            ((pool_hbm, pool_v), (prompt_hbm, prompt_v), (wo_hbm, wo_v))
        )
    ]
    for copy in small[:4]:
        copy.wait()

    values = hidden_v[...].astype(F32)
    scale = lax.rsqrt(jnp.mean(values * values, axis=-1, keepdims=True) + EPS)
    normed = (values * scale * gain_v[...]).astype(BF16)

    length_row = length_v[...].astype(F32)
    at = iota((rows, requests), 0) + me * rows
    own_length = jnp.sum(
        jnp.where(at == iota((rows, requests), 1), length_row, 0.0), axis=1, keepdims=True
    )
    angles = (own_length + float(prompt)) * freq_v[...]
    cosine = jnp.cos(angles)
    sine = jnp.sin(angles)
    half = HD // 2
    sine = jnp.where(iota(sine.shape, 1) < half, -sine, sine)

    heads = wq_v.shape[1] // HD
    query = jnp.zeros((rows, wq_v.shape[1]), F32)
    key = jnp.zeros((rows, HD), F32)
    value = jnp.zeros((rows, HD), F32)
    for i in range(pieces):
        for copy in weights[i]:
            copy.wait()
        if i == pieces - 1:
            for copy in bulk:
                copy.start()
        part = slice(i * depth, (i + 1) * depth)
        left = normed[:, part]
        query = query + dot(left, wq_v[part])
        key = key + dot(left, wk_v[part])
        value = value + dot(left, wv_v[part])

    def rope(x):
        return (x * cosine + pltpu.roll(x, half, 1) * sine).astype(BF16)

    own_query = [rope(query[:, h * HD : (h + 1) * HD]) for h in range(heads)]
    new_key = rope(key)
    new_value = value.astype(BF16)
    all_query[me] = jnp.concatenate(own_query, axis=1)

    pl.semaphore_wait(barrier, seq + tensor - 2)
    q_copies = []
    for d in farthest_first(seq):
        copy = pltpu.make_async_remote_copy(
            src_ref=all_query.at[me],
            dst_ref=all_query.at[me],
            send_sem=q_send_sem.at[d],
            recv_sem=q_recv_sem.at[d],
            device_id={"seq": seq_peer(d)},
            device_id_type=MESH,
        )
        copy.start()
        q_copies.append((d, copy))

    fresh_ref[:, 0, :] = new_key
    fresh_ref[:, 1, :] = new_value

    key32 = new_key.astype(F32)
    value32 = new_value.astype(F32)
    self_weight = [
        weigh(jnp.sum(q.astype(F32) * key32, axis=1, keepdims=True)) for q in own_query
    ]
    self_mix = [w.astype(BF16).astype(F32) * value32 for w in self_weight]

    small[4].wait()
    small[5].wait()
    turned = table_v[...].astype(F32).T
    page_id = (iota((pages, requests), 0) + me * pages).astype(F32)
    live = jnp.zeros((pages, requests), F32)
    for j in range(blocks):
        live = jnp.where(turned[j : j + 1, :] == page_id, length_row - float(j * block), live)
    owner = jnp.where(live > 0.0, 1.0, 0.0)
    valid = jnp.minimum(jnp.sum(live, axis=1, keepdims=True), float(block))
    owner_t = owner.T.astype(BF16)
    owner = owner.astype(BF16)

    same = iota((requests, requests), 0) == iota((requests, requests), 1)
    task = jnp.sum(
        jnp.where(same, task_v[...].astype(F32), 0.0), axis=1, keepdims=True
    ).astype(jnp.int32) - me * tasks

    for d, copy in q_copies:
        pltpu.make_async_remote_copy(
            src_ref=all_query.at[seq_from(d)],
            dst_ref=all_query.at[seq_from(d)],
            send_sem=q_send_sem.at[d],
            recv_sem=q_recv_sem.at[d],
            device_id={"seq": seq_from(d)},
            device_id_type=MESH,
        ).wait_recv()
    queries = all_query[...].reshape(requests, heads * HD)

    page_query = dot(owner, queries)
    bulk[0].wait()
    group = 8
    span = group * block
    lane = iota((heads * group, span), 1)
    row = lax.rem(iota((heads * group, span), 0), group)
    own_page = lax.div(lane, block) == row
    token = lax.rem(lane, block).astype(F32)
    token = jnp.where(own_page, token, float(2 * block))
    for g in range(pages // group):
        part = slice(g * group, (g + 1) * group)
        left = jnp.concatenate(
            [page_query[part, h * HD : (h + 1) * HD] for h in range(heads)], axis=0
        ).astype(BF16)
        count = jnp.concatenate([valid[part]] * heads, axis=0)
        raw = dot(left, pool_v[part, 0].reshape(span, HD), NT)
        weight = jnp.where(token < count, weigh(raw), 0.0)
        total = jnp.sum(weight, axis=1, keepdims=True)
        mix = dot(weight.astype(BF16), pool_v[part, 1].reshape(span, HD))
        for h in range(heads):
            page_mix[part, h * HD : (h + 1) * HD] = mix[h * group : (h + 1) * group]
        first = iota((group, HD), 1) < HD // heads
        page_mix[part, heads * HD :] = jnp.where(first, total[:group], total[group:])
    spread = dot(owner_t, page_mix[...].astype(BF16))

    bulk[1].wait()
    chunk = 8
    keys = chunk * prompt
    lane_task = lax.div(iota((requests, keys), 1), prompt)
    totals = []
    for h in range(heads):
        left = queries[:, h * HD : (h + 1) * HD]
        total = jnp.zeros((requests, 1), F32)
        mix = spread[:, h * HD : (h + 1) * HD]
        for b in range(tasks // chunk):
            part = slice(b * chunk, (b + 1) * chunk)
            raw = dot(left, prompt_v[part, 0].reshape(keys, HD), NT)
            weight = jnp.where(lane_task == task - b * chunk, weigh(raw), 0.0)
            total = total + jnp.sum(weight, axis=1, keepdims=True)
            mix = mix + dot(weight.astype(BF16), prompt_v[part, 1].reshape(keys, HD))
        mix_send[:, :, h * HD : (h + 1) * HD] = mix.astype(BF16).reshape(seq, rows, HD)
        totals.append(total)
    first = iota((requests, HD), 1) < HD // heads
    mix_send[:, :, heads * HD :] = (
        (spread[:, heads * HD :] + jnp.where(first, totals[0], totals[1]))
        .astype(BF16)
        .reshape(seq, rows, HD)
    )

    m_copies = []
    for d in farthest_first(seq):
        copy = pltpu.make_async_remote_copy(
            src_ref=mix_send.at[seq_peer(d)],
            dst_ref=mix_recv.at[d],
            send_sem=m_send_sem.at[d],
            recv_sem=m_recv_sem.at[d],
            device_id={"seq": seq_peer(d)},
            device_id_type=MESH,
        )
        copy.start()
        m_copies.append(copy)
    whole = mix_send[me].astype(F32)
    bulk[2].wait()
    small[6].wait()
    for copy in m_copies:
        copy.wait_recv()
    for d in range(1, seq):
        whole = whole + mix_recv[d].astype(F32)
    attended = []
    for h in range(heads):
        at = heads * HD + h * (HD // heads)
        total = whole[:, at : at + 1] + self_weight[h]
        mix = whole[:, h * HD : (h + 1) * HD] + self_mix[h]
        attended.append((mix / total).astype(BF16))
    projected = dot(jnp.concatenate(attended, axis=1), wo_v[...])

    tail = cols % HD
    full = cols // HD
    fold = HD // tail
    step = rows // fold
    for k in range(tensor):
        piece = projected[:, k * cols : (k + 1) * cols]
        for f in range(full):
            proj_send[k, f * rows : (f + 1) * rows] = piece[:, f * HD : (f + 1) * HD].astype(BF16)
        end = piece[:, full * HD :]
        proj_send[k, full * rows :] = jnp.concatenate(
            [end[i * step : (i + 1) * step] for i in range(fold)], axis=1
        ).astype(BF16)
    p_copies = []
    for d in farthest_first(tensor):
        copy = pltpu.make_async_remote_copy(
            src_ref=proj_send.at[tensor_peer(d)],
            dst_ref=proj_recv.at[d],
            send_sem=p_send_sem.at[d],
            recv_sem=p_recv_sem.at[d],
            device_id={"tensor": tensor_peer(d)},
            device_id_type=MESH,
        )
        copy.start()
        p_copies.append(copy)
    share = proj_send[mine].astype(F32)
    start = mine * cols
    base = lax.div(start, HD) * HD
    reach = (full + 1) * HD
    residual = hidden_v[:, pl.ds(pl.multiple_of(base, HD), reach)].astype(F32)
    residual = pltpu.roll(residual, lax.rem(reach - (start - base), reach), 1)
    for copy in p_copies:
        copy.wait_recv()
    for d in range(1, tensor):
        share = share + proj_recv[d].astype(F32)

    squares = share * share
    body_sum = squares[:rows]
    for f in range(1, full):
        body_sum = body_sum + squares[f * rows : (f + 1) * rows]
    body_sum = jnp.sum(body_sum, axis=1, keepdims=True)
    ends = squares[full * rows :]
    lane = iota((step, HD), 1)
    down = iota((step, HD), 0)
    line = jnp.zeros((step, HD), F32)
    for i in range(fold):
        of_end = jnp.sum(
            jnp.where(lax.div(lane, tail) == i, ends, 0.0), axis=1, keepdims=True
        )
        line = jnp.where(
            lane == i * tail + down, body_sum[i * step : (i + 1) * step] + of_end, line
        )
    square[0] = jnp.sum(line, axis=0, keepdims=True)
    s_copies = []
    for d in farthest_first(tensor):
        copy = pltpu.make_async_remote_copy(
            src_ref=square.at[0],
            dst_ref=square.at[d],
            send_sem=s_send_sem.at[d],
            recv_sem=s_recv_sem.at[d],
            device_id={"tensor": tensor_peer(d)},
            device_id_type=MESH,
        )
        copy.start()
        s_copies.append(copy)
    for copy in s_copies:
        copy.wait_recv()
    summed = square[0]
    for d in range(1, tensor):
        summed = summed + square[d]
    inverse = lax.rsqrt(summed * (1.0 / width) + EPS)
    columns = [
        jnp.sum(jnp.where(lane == i * tail + down, inverse, 0.0), axis=1, keepdims=True)
        for i in range(fold)
    ]
    post = post_v[...]
    inverse = jnp.concatenate(columns, axis=0)
    for f in range(full):
        part = slice(f * HD, (f + 1) * HD)
        out_ref[:, part] = (
            residual[:, part] + share[f * rows : (f + 1) * rows] * inverse * post[:, part]
        ).astype(BF16)
    end = jnp.concatenate(
        [share[full * rows :, i * tail : (i + 1) * tail] for i in range(fold)], axis=0
    )
    out_ref[:, full * HD :] = (
        residual[:, full * HD : cols] + end * inverse * post[:, full * HD :]
    ).astype(BF16)

    for _, copy in q_copies:
        copy.wait_send()
    for copy in m_copies + p_copies + s_copies:
        copy.wait_send()


def body(
    seq,
    tensor,
    hidden,
    pre_gain,
    w_query,
    w_key,
    w_value,
    w_out,
    post_gain,
    cache_pool,
    prompt_cache,
    task_ids,
    cache_lengths,
    block_table,
):
    rows, width = hidden.shape
    cols = post_gain.shape[0]
    heads = w_query.shape[1] // HD
    pages = cache_pool.shape[0]
    lines = rows * cols // HD
    pieces = 6
    half = HD // 2
    freq = np.float32(10000.0) ** (-np.arange(half, dtype=np.float64) / half)
    freq = jnp.asarray(np.concatenate([freq, freq])[None].astype(np.float32))
    args = (
        hidden,
        pre_gain.reshape(1, -1),
        w_query,
        w_key,
        w_value,
        w_out,
        post_gain.reshape(1, -1),
        cache_pool,
        prompt_cache,
        task_ids.reshape(1, -1),
        cache_lengths.reshape(1, -1),
        block_table,
        freq,
    )
    wide = (heads + 1) * HD
    dma = pltpu.SemaphoreType.DMA
    return pl.pallas_call(
        functools.partial(layer, seq=seq, tensor=tensor, pieces=pieces),
        out_shape=(
            jax.ShapeDtypeStruct((rows, cols), BF16),
            jax.ShapeDtypeStruct((rows, 2, HD), BF16),
        ),
        in_specs=[pl.BlockSpec(memory_space=pltpu.HBM)] * len(args),
        out_specs=[pl.BlockSpec(memory_space=pltpu.VMEM)] * 2,
        scratch_shapes=[pltpu.VMEM(a.shape, a.dtype) for a in args]
        + [
            pltpu.VMEM((pages, wide), F32),
            pltpu.VMEM((seq, rows, heads * HD), BF16),
            pltpu.VMEM((seq, rows, wide), BF16),
            pltpu.VMEM((seq, rows, wide), BF16),
            pltpu.VMEM((tensor, lines, HD), BF16),
            pltpu.VMEM((tensor, lines, HD), BF16),
            pltpu.VMEM((tensor, 1, HD), F32),
            dma((10,)),
            dma((3 * pieces,)),
            dma((seq,)),
            dma((seq,)),
            dma((seq,)),
            dma((seq,)),
            dma((tensor,)),
            dma((tensor,)),
            dma((tensor,)),
            dma((tensor,)),
        ],
        compiler_params=pltpu.CompilerParams(
            collective_id=0, has_side_effects=True, vmem_limit_bytes=60 * 1024 * 1024
        ),
        name="layer",
    )(*args)


def solution(mesh):
    seq = mesh.shape["seq"]
    tensor = mesh.shape["tensor"]
    return jax.shard_map(
        functools.partial(body, seq, tensor),
        mesh=mesh,
        in_specs=(
            P(("groups", "seq"), None),
            P(),
            P(None, "tensor"),
            P(None, "tensor"),
            P(None, "tensor"),
            P("tensor", None),
            P("tensor"),
            P(("groups", "seq"), None, None, "tensor"),
            P("seq", None, None, "tensor"),
            P("groups"),
            P("groups"),
            P("groups", None),
        ),
        out_specs=(P(("groups", "seq"), "tensor"), P(("groups", "seq"), None, "tensor")),
        check_vma=False,
    )
```

```python
import functools
import math

import jax
import jax.numpy as jnp
import numpy as np
from jax import lax
from jax.experimental import pallas as pl
from jax.experimental.pallas import tpu as pltpu
from jax.sharding import PartitionSpec as P

D = 4608
H = 32
HD = 128
CAP = 50.0
EPS = 1e-6
MESH = pl.DeviceIdType.MESH
F32 = jnp.float32
BF16 = jnp.bfloat16
NT = (((1,), (1,)), ((), ()))
NN = (((1,), (0,)), ((), ()))

INNER = float(D // H) ** (-0.5) / CAP
OUTER = CAP * math.log2(math.e)


def dot(a, b, dims=NN):
    return lax.dot_general(a, b, dims, preferred_element_type=F32)


def weigh(raw):
    return jnp.exp2(OUTER * jnp.tanh(raw * INNER))


def iota(shape, dim):
    return lax.broadcasted_iota(jnp.int32, shape, dim)


def spread_lanes(columns, lane):
    width = lane.shape[1] // len(columns)
    out = jnp.broadcast_to(columns[0], lane.shape)
    for i in range(1, len(columns)):
        out = jnp.where(lane >= i * width, columns[i], out)
    return out


def farthest_first(size):
    return sorted(range(1, size), key=lambda d: -min(d, size - d))


def layer(
    hidden_hbm,
    gain_hbm,
    wq_hbm,
    wk_hbm,
    wv_hbm,
    wo_hbm,
    post_hbm,
    pool_hbm,
    prompt_hbm,
    task_hbm,
    length_hbm,
    table_hbm,
    freq_hbm,
    out_ref,
    fresh_ref,
    hidden_v,
    gain_v,
    wq_v,
    wk_v,
    wv_v,
    wo_v,
    post_v,
    pool_v,
    prompt_v,
    task_v,
    length_v,
    table_v,
    freq_v,
    page_mix,
    prompt_mix,
    prompt_total,
    task_column,
    all_query,
    mix_send,
    mix_recv,
    proj_send,
    proj_recv,
    square,
    here,
    in_sem,
    w_sem,
    q_send_sem,
    q_recv_sem,
    m_send_sem,
    m_recv_sem,
    p_send_sem,
    p_recv_sem,
    s_send_sem,
    s_recv_sem,
    *,
    seq,
    tensor,
    pieces,
):
    me = lax.axis_index("seq")
    mine = lax.axis_index("tensor")
    rows, width = hidden_v.shape
    requests = task_v.shape[1]
    pages = pool_v.shape[0]
    block = pool_v.shape[2]
    tasks, _, prompt, _ = prompt_v.shape
    blocks = table_v.shape[0]
    cols = out_ref.shape[1]

    chips = seq // 2
    chip, core = lax.div(me, 2), lax.rem(me, 2)
    slot = lambda ahead, other: lax.rem(chip + ahead, chips) * 2 + lax.rem(core + other, 2)
    source = lambda ahead, other: slot((chips - ahead) % chips, other)
    routes = [
        (ahead, other)
        for ahead in farthest_first(chips) + [0]
        for other in (1, 0)
        if ahead + other > 0
    ]
    tensor_peer = lambda d: lax.rem(mine + d, tensor)

    at_place = lambda p: (p + 1) % tensor
    place = lax.rem(mine + tensor - 1, tensor)

    barrier = pltpu.get_barrier_semaphore()
    for route in routes:
        pl.semaphore_signal(barrier, inc=1, device_id={"seq": slot(*route)}, device_id_type=MESH)
    for p in range(1, tensor):

        @pl.when(place < p)
        def _(p=p):
            pl.semaphore_signal(
                barrier, inc=1, device_id={"tensor": at_place(p)}, device_id_type=MESH
            )

    small = [
        pltpu.make_async_copy(src, dst, in_sem.at[i])
        for i, (src, dst) in enumerate(
            (
                (hidden_hbm, hidden_v),
                (gain_hbm, gain_v),
                (length_hbm, length_v),
                (freq_hbm, freq_v),
                (table_hbm, table_v),
                (task_hbm, task_v),
                (post_hbm, post_v),
            )
        )
    ]
    for copy in small:
        copy.start()
    depth = width // pieces
    weights = []
    for i in range(pieces):
        part = pl.ds(i * depth, depth)
        weights.append(
            [
                pltpu.make_async_copy(src.at[part], dst.at[part], w_sem.at[3 * i + j])
                for j, (src, dst) in enumerate(
                    ((wq_hbm, wq_v), (wk_hbm, wk_v), (wv_hbm, wv_v))
                )
            ]
        )
    for group in weights[: pieces // 2]:
        for copy in group:
            copy.start()
    bulk = [
        pltpu.make_async_copy(src, dst, in_sem.at[len(small) + i])
        for i, (src, dst) in enumerate(
            ((pool_hbm, pool_v), (prompt_hbm, prompt_v), (wo_hbm, wo_v))
        )
    ]

    for copy in small[:4]:
        copy.wait()
    for group in weights[pieces // 2 :]:
        for copy in group:
            copy.start()

    values = hidden_v[...].astype(F32)
    scale = lax.rsqrt(jnp.mean(values * values, axis=-1, keepdims=True) + EPS)
    normed = (values * scale * gain_v[...].reshape(1, -1)).astype(BF16)

    length_row = length_v[...].astype(F32)
    at = iota((rows, requests), 0) + me * rows
    own_length = jnp.sum(
        jnp.where(at == iota((rows, requests), 1), length_row, 0.0), axis=1, keepdims=True
    )
    angles = (own_length + float(prompt)) * freq_v[...]
    cosine = jnp.cos(angles)
    sine = jnp.sin(angles)
    half = HD // 2
    sine = jnp.where(iota(sine.shape, 1) < half, -sine, sine)

    heads = wq_v.shape[1] // HD
    query = jnp.zeros((rows, wq_v.shape[1]), F32)
    key = jnp.zeros((rows, HD), F32)
    value = jnp.zeros((rows, HD), F32)
    for i in range(pieces):
        for copy in weights[i]:
            copy.wait()
        if i == pieces - 1:
            for copy in bulk:
                copy.start()
        part = slice(i * depth, (i + 1) * depth)
        left = normed[:, part]
        query = query + dot(left, wq_v[part])
        key = key + dot(left, wk_v[part])
        value = value + dot(left, wv_v[part])

    def rope(x):
        return (x * cosine + pltpu.roll(x, half, 1) * sine).astype(BF16)

    own_query = [rope(query[:, h * HD : (h + 1) * HD]) for h in range(heads)]
    new_key = rope(key)
    new_value = value.astype(BF16)
    all_query[me] = jnp.concatenate(own_query, axis=1)

    pl.semaphore_wait(barrier, seq - 1 + place)
    for p in range(tensor - 1):

        @pl.when(p < place)
        def _(p=p):
            pl.semaphore_signal(
                here.at[place], inc=1, device_id={"tensor": at_place(p)}, device_id_type=MESH
            )

    q_copies = {}
    for ahead, other in routes:
        q_copies[ahead, other] = pltpu.make_async_remote_copy(
            src_ref=all_query.at[me],
            dst_ref=all_query.at[me],
            send_sem=q_send_sem.at[2 * ahead + other],
            recv_sem=q_recv_sem.at[2 * ahead + other],
            device_id={"seq": slot(ahead, other)},
            device_id_type=MESH,
        )
        q_copies[ahead, other].start()

    fresh_ref[:, 0, :] = new_key
    fresh_ref[:, 1, :] = new_value

    key32 = new_key.astype(F32)
    value32 = new_value.astype(F32)
    self_weight = [
        weigh(jnp.sum(q.astype(F32) * key32, axis=1, keepdims=True)) for q in own_query
    ]
    self_mix = [w.astype(BF16).astype(F32) * value32 for w in self_weight]

    small[5].wait()
    same = iota((requests, requests), 0) == iota((requests, requests), 1)
    task = jnp.sum(
        jnp.where(same, task_v[...].astype(F32), 0.0), axis=1, keepdims=True
    ).astype(jnp.int32) - me * tasks
    task_column[...] = jnp.broadcast_to(task, (requests, HD)).reshape(seq, rows, HD)

    chunk = 8
    keys = chunk * prompt

    def attend_prompts(slots):
        left = jnp.concatenate(
            [all_query[s, :, h * HD : (h + 1) * HD] for s in slots for h in range(heads)], axis=0
        )
        wanted = jnp.concatenate(
            [task_column[s, :, :1] for s in slots for h in range(heads)], axis=0
        )
        count = left.shape[0]
        lane_task = lax.div(iota((count, keys), 1), prompt)
        total = jnp.zeros((count, 1), F32)
        mix = jnp.zeros((count, HD), F32)
        for b in range(tasks // chunk):
            part = slice(b * chunk, (b + 1) * chunk)
            raw = dot(left, prompt_v[part, 0].reshape(keys, HD), NT)
            weight = jnp.where(lane_task == wanted - b * chunk, weigh(raw), 0.0)
            total = total + jnp.sum(weight, axis=1, keepdims=True)
            mix = mix + dot(weight.astype(BF16), prompt_v[part, 1].reshape(keys, HD))
        span = heads * rows
        for i, s in enumerate(slots):
            prompt_mix[s] = mix[i * span : (i + 1) * span]
            prompt_total[s] = jnp.broadcast_to(total[i * span : (i + 1) * span], (span, HD))

    def arrive(route):
        came = source(*route)
        pltpu.make_async_remote_copy(
            src_ref=all_query.at[came],
            dst_ref=all_query.at[came],
            send_sem=q_send_sem.at[2 * route[0] + route[1]],
            recv_sem=q_recv_sem.at[2 * route[0] + route[1]],
            device_id={"seq": came},
            device_id_type=MESH,
        ).wait_recv()
        return came

    bulk[1].wait()
    attend_prompts([me])

    small[4].wait()
    turned = table_v[...].astype(F32)
    page_id = (iota((pages, requests), 0) + me * pages).astype(F32)
    live = jnp.zeros((pages, requests), F32)
    for j in range(blocks):
        live = jnp.where(turned[j : j + 1, :] == page_id, length_row - float(j * block), live)
    owner = jnp.where(live > 0.0, 1.0, 0.0)
    valid = jnp.minimum(jnp.sum(live, axis=1, keepdims=True), float(block))
    owner_t = owner.T.astype(BF16)
    owner = owner.astype(BF16)

    far = farthest_first(chips)
    arrivals = [[(0, 1)], [(a, o) for a in far if a in (1, chips - 1) for o in (0, 1)]]
    rest = [(a, o) for a in far if a not in (1, chips - 1) for o in (0, 1)]
    if rest:
        arrivals.append(rest)
    for batch in arrivals:
        attend_prompts([arrive(route) for route in batch])
    queries = all_query[...].reshape(requests, heads * HD)

    page_query = dot(owner, queries)
    bulk[0].wait()
    group = 8
    span = group * block
    lane = iota((heads * group, span), 1)
    row = lax.rem(iota((heads * group, span), 0), group)
    own_page = lax.div(lane, block) == row
    token = lax.rem(lane, block).astype(F32)
    token = jnp.where(own_page, token, float(2 * block))
    for g in range(pages // group):
        part = slice(g * group, (g + 1) * group)
        left = jnp.concatenate(
            [page_query[part, h * HD : (h + 1) * HD] for h in range(heads)], axis=0
        ).astype(BF16)
        count = jnp.concatenate([valid[part]] * heads, axis=0)
        raw = dot(left, pool_v[part, 0].reshape(span, HD), NT)
        weight = jnp.where(token < count, weigh(raw), 0.0)
        total = jnp.sum(weight, axis=1, keepdims=True)
        mix = dot(weight.astype(BF16), pool_v[part, 1].reshape(span, HD))
        for h in range(heads):
            page_mix[part, h * HD : (h + 1) * HD] = mix[h * group : (h + 1) * group]
        high = total.astype(BF16).astype(F32)
        low = total - high
        fine = iota((group, HD), 1)
        columns = [x[h * group : (h + 1) * group] for h in range(heads) for x in (high, low)]
        page_mix[part, heads * HD :] = spread_lanes(columns, fine)
    spread = dot(owner_t, page_mix[...].astype(BF16))

    lanes = HD // (2 * heads)
    sums = []
    for h in range(heads):
        part = slice(h * rows, (h + 1) * rows)
        mix_send[:, part] = (
            spread[:, h * HD : (h + 1) * HD].reshape(seq, rows, HD) + prompt_mix[:, part]
        ).astype(BF16)
        at = heads * HD + 2 * h * lanes
        sums.append(
            spread[:, at : at + 1]
            + spread[:, at + lanes : at + lanes + 1]
            + prompt_total[:, part, :1].reshape(requests, 1)
        )
    fine = iota((8, HD), 1)
    for j in range(seq):
        columns = []
        for h in range(heads):
            for q in range(rows // 8):
                total = sums[h][j * rows + q * 8 : j * rows + q * 8 + 8]
                high = total.astype(BF16).astype(F32)
                columns += [high, total - high]
        mix_send[j, heads * rows :] = spread_lanes(columns, fine).astype(BF16)

    m_copies = []
    for ahead, other in routes:
        copy = pltpu.make_async_remote_copy(
            src_ref=mix_send.at[slot(ahead, other)],
            dst_ref=mix_recv.at[2 * ahead + other],
            send_sem=m_send_sem.at[2 * ahead + other],
            recv_sem=m_recv_sem.at[2 * ahead + other],
            device_id={"seq": slot(ahead, other)},
            device_id_type=MESH,
        )
        copy.start()
        m_copies.append(copy)
    whole = mix_send[me].astype(F32)
    bulk[2].wait()
    small[6].wait()
    for copy in m_copies:
        copy.wait_recv()
    for d in range(1, seq):
        whole = whole + mix_recv[d].astype(F32)
    table = whole[heads * rows :]
    attended = []
    for h in range(heads):
        line = rows // 8
        lanes = HD // (2 * heads * line)
        total = jnp.concatenate(
            [
                table[:, (2 * q) * lanes : (2 * q) * lanes + 1]
                + table[:, (2 * q + 1) * lanes : (2 * q + 1) * lanes + 1]
                for q in range(h * line, (h + 1) * line)
            ],
            axis=0,
        )
        total = total + self_weight[h]
        mix = whole[h * rows : (h + 1) * rows] + self_mix[h]
        attended.append((mix / total).astype(BF16))
    projected = dot(jnp.concatenate(attended, axis=1), wo_v[...])

    tail = cols % HD
    full = cols // HD
    fold = HD // tail
    step = rows // fold
    for k in range(tensor):
        piece = projected[:, k * cols : (k + 1) * cols]
        for f in range(full):
            proj_send[k, f * rows : (f + 1) * rows] = piece[:, f * HD : (f + 1) * HD].astype(BF16)
        end = piece[:, full * HD :]
        proj_send[k, full * rows :] = jnp.concatenate(
            [end[i * step : (i + 1) * step] for i in range(fold)], axis=1
        ).astype(BF16)
    p_copies = [
        pltpu.make_async_remote_copy(
            src_ref=proj_send.at[tensor_peer(d)],
            dst_ref=proj_recv.at[d],
            send_sem=p_send_sem.at[d],
            recv_sem=p_recv_sem.at[d],
            device_id={"tensor": tensor_peer(d)},
            device_id_type=MESH,
        )
        for d in range(1, tensor)
    ]
    for d in farthest_first(tensor):

        @pl.when(place + d < tensor)
        def _(d=d):
            pl.semaphore_wait(here.at[place + d], 1)

        p_copies[d - 1].start()
    share = proj_send[mine].astype(F32)
    start = mine * cols
    base = lax.div(start, HD) * HD
    reach = (full + 1) * HD
    residual = hidden_v[:, pl.ds(pl.multiple_of(base, HD), reach)].astype(F32)
    residual = pltpu.roll(residual, lax.rem(reach - (start - base), reach), 1)
    for copy in p_copies:
        copy.wait_recv()
    for d in range(1, tensor):
        share = share + proj_recv[d].astype(F32)

    squares = share * share
    body_sum = squares[:rows]
    for f in range(1, full):
        body_sum = body_sum + squares[f * rows : (f + 1) * rows]
    body_sum = jnp.sum(body_sum, axis=1, keepdims=True)
    ends = squares[full * rows :]
    lane = iota((step, HD), 1)
    down = iota((step, HD), 0)
    line = jnp.zeros((step, HD), F32)
    for i in range(fold):
        of_end = jnp.sum(
            jnp.where(lax.div(lane, tail) == i, ends, 0.0), axis=1, keepdims=True
        )
        line = jnp.where(
            lane == i * tail + down, body_sum[i * step : (i + 1) * step] + of_end, line
        )
    square[0] = jnp.sum(line, axis=0, keepdims=True)
    s_copies = []
    for d in farthest_first(tensor):
        copy = pltpu.make_async_remote_copy(
            src_ref=square.at[0],
            dst_ref=square.at[d],
            send_sem=s_send_sem.at[d],
            recv_sem=s_recv_sem.at[d],
            device_id={"tensor": tensor_peer(d)},
            device_id_type=MESH,
        )
        copy.start()
        s_copies.append(copy)
    for copy in s_copies:
        copy.wait_recv()
    summed = square[0]
    for d in range(1, tensor):
        summed = summed + square[d]
    inverse = lax.rsqrt(summed * (1.0 / width) + EPS)
    columns = [
        jnp.sum(jnp.where(lane == i * tail + down, inverse, 0.0), axis=1, keepdims=True)
        for i in range(fold)
    ]
    post = post_v[...].reshape(1, -1)
    inverse = jnp.concatenate(columns, axis=0)
    for f in range(full):
        part = slice(f * HD, (f + 1) * HD)
        out_ref[:, part] = (
            residual[:, part] + share[f * rows : (f + 1) * rows] * inverse * post[:, part]
        ).astype(BF16)
    end = jnp.concatenate(
        [share[full * rows :, i * tail : (i + 1) * tail] for i in range(fold)], axis=0
    )
    out_ref[:, full * HD :] = (
        residual[:, full * HD : cols] + end * inverse * post[:, full * HD :]
    ).astype(BF16)

    for copy in q_copies.values():
        copy.wait_send()
    for copy in m_copies + p_copies + s_copies:
        copy.wait_send()


def hand_out(out_ref, fresh_ref, out, fresh):
    out[...] = out_ref[...]
    fresh[...] = fresh_ref[...]


def body(
    seq,
    tensor,
    hidden,
    pre_gain,
    w_query,
    w_key,
    w_value,
    w_out,
    post_gain,
    cache_pool,
    prompt_cache,
    task_ids,
    cache_lengths,
    block_table,
):
    rows, width = hidden.shape
    cols = post_gain.shape[0]
    heads = w_query.shape[1] // HD
    pages = cache_pool.shape[0]
    lines = rows * cols // HD
    pieces = 6
    half = HD // 2
    freq = np.float32(10000.0) ** (-np.arange(half, dtype=np.float64) / half)
    freq = jnp.asarray(np.concatenate([freq, freq])[None].astype(np.float32))
    args = (
        hidden,
        pre_gain,
        w_query,
        w_key,
        w_value,
        w_out,
        post_gain,
        cache_pool,
        prompt_cache,
        task_ids.reshape(1, -1),
        cache_lengths.reshape(1, -1),
        block_table.T,
        freq,
    )
    wide = (heads + 1) * HD
    dma = pltpu.SemaphoreType.DMA
    outs = pl.pallas_call(
        functools.partial(layer, seq=seq, tensor=tensor, pieces=pieces),
        out_shape=(
            pltpu.VMEM((rows, cols), BF16),
            pltpu.VMEM((rows, 2, HD), BF16),
        ),
        in_specs=[pl.BlockSpec(memory_space=pltpu.HBM)] * len(args),
        out_specs=[pl.BlockSpec(memory_space=pltpu.VMEM)] * 2,
        scratch_shapes=[pltpu.VMEM(a.shape, a.dtype) for a in args]
        + [
            pltpu.VMEM((pages, wide), F32),
            pltpu.VMEM((seq, heads * rows, HD), F32),
            pltpu.VMEM((seq, heads * rows, HD), F32),
            pltpu.VMEM((seq, rows, HD), jnp.int32),
            pltpu.VMEM((seq, rows, heads * HD), BF16),
            pltpu.VMEM((seq, heads * rows + 8, HD), BF16),
            pltpu.VMEM((seq, heads * rows + 8, HD), BF16),
            pltpu.VMEM((tensor, lines, HD), BF16),
            pltpu.VMEM((tensor, lines, HD), BF16),
            pltpu.VMEM((tensor, 1, HD), F32),
            pltpu.SemaphoreType.REGULAR((tensor,)),
            dma((10,)),
            dma((3 * pieces,)),
            dma((seq,)),
            dma((seq,)),
            dma((seq,)),
            dma((seq,)),
            dma((tensor,)),
            dma((tensor,)),
            dma((tensor,)),
            dma((tensor,)),
        ],
        compiler_params=pltpu.CompilerParams(
            collective_id=0, has_side_effects=True, vmem_limit_bytes=60 * 1024 * 1024
        ),
        name="layer",
    )(*args)
    return pl.pallas_call(
        hand_out,
        out_shape=tuple(jax.ShapeDtypeStruct(a.shape, a.dtype) for a in outs),
        in_specs=[pl.BlockSpec(memory_space=pltpu.VMEM)] * 2,
        out_specs=[pl.BlockSpec(memory_space=pltpu.VMEM)] * 2,
        name="hand_out",
    )(*(pltpu.with_memory_space_constraint(a, pltpu.VMEM) for a in outs))


def solution(mesh):
    seq = mesh.shape["seq"]
    tensor = mesh.shape["tensor"]
    return jax.shard_map(
        functools.partial(body, seq, tensor),
        mesh=mesh,
        in_specs=(
            P(("groups", "seq"), None),
            P(),
            P(None, "tensor"),
            P(None, "tensor"),
            P(None, "tensor"),
            P("tensor", None),
            P("tensor"),
            P(("groups", "seq"), None, None, "tensor"),
            P("seq", None, None, "tensor"),
            P("groups"),
            P("groups"),
            P("groups", None),
        ),
        out_specs=(P(("groups", "seq"), "tensor"), P(("groups", "seq"), None, "tensor")),
        check_vma=False,
    )
```

```python
import functools
import math

import jax
import jax.numpy as jnp
import numpy as np
from jax import lax
from jax.experimental import pallas as pl
from jax.experimental.pallas import tpu as pltpu
from jax.sharding import PartitionSpec as P

D = 4608
H = 32
HD = 128
CAP = 50.0
EPS = 1e-6
MESH = pl.DeviceIdType.MESH
F32 = jnp.float32
BF16 = jnp.bfloat16
NT = (((1,), (1,)), ((), ()))
NN = (((1,), (0,)), ((), ()))

INNER = float(D // H) ** (-0.5) / CAP
OUTER = CAP * math.log2(math.e)


def dot(a, b, dims=NN):
    return lax.dot_general(a, b, dims, preferred_element_type=F32)


def weigh(raw):
    return jnp.exp2(OUTER * jnp.tanh(raw * INNER))


def iota(shape, dim):
    return lax.broadcasted_iota(jnp.int32, shape, dim)


def spread_lanes(columns, lane):
    width = lane.shape[1] // len(columns)
    out = jnp.broadcast_to(columns[0], lane.shape)
    for i in range(1, len(columns)):
        out = jnp.where(lane >= i * width, columns[i], out)
    return out


def farthest_first(size):
    return sorted(range(1, size), key=lambda d: -min(d, size - d))


def layer(
    hidden_hbm,
    gain_hbm,
    wq_hbm,
    wk_hbm,
    wv_hbm,
    wo_hbm,
    post_hbm,
    pool_hbm,
    prompt_hbm,
    task_hbm,
    length_hbm,
    table_hbm,
    freq_hbm,
    out_ref,
    fresh_ref,
    hidden_v,
    gain_v,
    wq_v,
    wk_v,
    wv_v,
    wo_v,
    post_v,
    pool_v,
    prompt_v,
    task_v,
    length_v,
    table_v,
    freq_v,
    page_mix,
    prompt_mix,
    prompt_total,
    task_column,
    all_query,
    mix_send,
    mix_recv,
    proj_send,
    proj_recv,
    square,
    here,
    in_sem,
    w_sem,
    q_send_sem,
    q_recv_sem,
    m_send_sem,
    m_recv_sem,
    p_send_sem,
    p_recv_sem,
    s_send_sem,
    s_recv_sem,
    *,
    seq,
    tensor,
    pieces,
):
    me = lax.axis_index("seq")
    mine = lax.axis_index("tensor")
    rows, width = hidden_v.shape
    requests = task_v.shape[1]
    pages = pool_v.shape[0]
    block = pool_v.shape[2]
    tasks, _, prompt, _ = prompt_v.shape
    blocks = table_v.shape[0]
    cols = out_ref.shape[1]

    chips = seq // 2
    chip, core = lax.div(me, 2), lax.rem(me, 2)
    slot = lambda ahead, other: lax.rem(chip + ahead, chips) * 2 + lax.rem(core + other, 2)
    source = lambda ahead, other: slot((chips - ahead) % chips, other)
    routes = [
        (ahead, other)
        for ahead in farthest_first(chips) + [0]
        for other in (1, 0)
        if ahead + other > 0
    ]
    tensor_peer = lambda d: lax.rem(mine + d, tensor)

    at_place = lambda p: (p + 1) % tensor
    place = lax.rem(mine + tensor - 1, tensor)

    barrier = pltpu.get_barrier_semaphore()
    for route in routes:
        pl.semaphore_signal(barrier, inc=1, device_id={"seq": slot(*route)}, device_id_type=MESH)
    for p in range(1, tensor):

        @pl.when(place < p)
        def _(p=p):
            pl.semaphore_signal(
                barrier, inc=1, device_id={"tensor": at_place(p)}, device_id_type=MESH
            )

    def arrived(ref, sem):
        pltpu.make_async_copy(ref, ref, sem).wait()

    small = [
        pltpu.make_async_copy(src, dst, in_sem.at[i])
        for i, (src, dst) in enumerate(
            (
                (hidden_hbm, hidden_v),
                (gain_hbm, gain_v),
                (length_hbm, length_v),
                (freq_hbm, freq_v),
                (table_hbm, table_v),
                (task_hbm, task_v),
                (post_hbm, post_v),
            )
        )
    ]
    for copy in small:
        copy.start()
    depth = width // pieces
    weights = []
    for i in range(pieces):
        part = pl.ds(i * depth, depth)
        weights.append(
            [
                pltpu.make_async_copy(src.at[part], dst.at[part], w_sem.at[i])
                for src, dst in ((wq_hbm, wq_v), (wk_hbm, wk_v), (wv_hbm, wv_v))
            ]
        )
    for group in weights[: pieces // 2]:
        for copy in group:
            copy.start()
    bulk = [
        pltpu.make_async_copy(src, dst, in_sem.at[len(small) + i])
        for i, (src, dst) in enumerate(
            ((pool_hbm, pool_v), (prompt_hbm, prompt_v), (wo_hbm, wo_v))
        )
    ]

    for copy in small[:4]:
        copy.wait()
    for group in weights[pieces // 2 :]:
        for copy in group:
            copy.start()

    values = hidden_v[...].astype(F32)
    scale = lax.rsqrt(jnp.mean(values * values, axis=-1, keepdims=True) + EPS)
    normed = (values * scale * gain_v[...].reshape(1, -1)).astype(BF16)

    length_row = length_v[...].astype(F32)
    at = iota((rows, requests), 0) + me * rows
    own_length = jnp.sum(
        jnp.where(at == iota((rows, requests), 1), length_row, 0.0), axis=1, keepdims=True
    )
    angles = (own_length + float(prompt)) * freq_v[...]
    cosine = jnp.cos(angles)
    sine = jnp.sin(angles)
    half = HD // 2
    sine = jnp.where(iota(sine.shape, 1) < half, -sine, sine)

    heads = wq_v.shape[1] // HD
    query = jnp.zeros((rows, wq_v.shape[1]), F32)
    key = jnp.zeros((rows, HD), F32)
    value = jnp.zeros((rows, HD), F32)
    for i in range(pieces):
        arrived(wq_v.at[pl.ds(0, 2 * depth)], w_sem.at[i])
        if i == pieces // 2:
            bulk[1].start()
        if i == pieces - 1:
            bulk[0].start()
            bulk[2].start()
        part = slice(i * depth, (i + 1) * depth)
        left = normed[:, part]
        query = query + dot(left, wq_v[part])
        key = key + dot(left, wk_v[part])
        value = value + dot(left, wv_v[part])

    def rope(x):
        return (x * cosine + pltpu.roll(x, half, 1) * sine).astype(BF16)

    own_query = [rope(query[:, h * HD : (h + 1) * HD]) for h in range(heads)]
    new_key = rope(key)
    new_value = value.astype(BF16)
    all_query[me] = jnp.concatenate(own_query, axis=1)

    pl.semaphore_wait(barrier, seq - 1 + place)
    for p in range(tensor - 1):

        @pl.when(p < place)
        def _(p=p):
            pl.semaphore_signal(
                here.at[place], inc=1, device_id={"tensor": at_place(p)}, device_id_type=MESH
            )

    q_copies = {}
    for ahead, other in routes:
        q_copies[ahead, other] = pltpu.make_async_remote_copy(
            src_ref=all_query.at[me],
            dst_ref=all_query.at[me],
            send_sem=q_send_sem,
            recv_sem=q_recv_sem.at[2 * ahead + other],
            device_id={"seq": slot(ahead, other)},
            device_id_type=MESH,
        )
        q_copies[ahead, other].start()

    fresh_ref[:, 0, :] = new_key
    fresh_ref[:, 1, :] = new_value

    key32 = new_key.astype(F32)
    value32 = new_value.astype(F32)
    self_weight = [
        weigh(jnp.sum(q.astype(F32) * key32, axis=1, keepdims=True)) for q in own_query
    ]
    self_mix = [w.astype(BF16).astype(F32) * value32 for w in self_weight]

    small[5].wait()
    same = iota((requests, requests), 0) == iota((requests, requests), 1)
    task = jnp.sum(
        jnp.where(same, task_v[...].astype(F32), 0.0), axis=1, keepdims=True
    ).astype(jnp.int32) - me * tasks
    task_column[...] = jnp.broadcast_to(task, (requests, HD)).reshape(seq, rows, HD)

    chunk = 8
    keys = chunk * prompt

    def attend_prompts(slots):
        left = jnp.concatenate(
            [all_query[s, :, h * HD : (h + 1) * HD] for s in slots for h in range(heads)], axis=0
        )
        wanted = jnp.concatenate(
            [task_column[s, :, :1] for s in slots for h in range(heads)], axis=0
        )
        count = left.shape[0]
        lane_task = lax.div(iota((count, keys), 1), prompt)
        total = jnp.zeros((count, 1), F32)
        mix = jnp.zeros((count, HD), F32)
        for b in range(tasks // chunk):
            part = slice(b * chunk, (b + 1) * chunk)
            raw = dot(left, prompt_v[part, 0].reshape(keys, HD), NT)
            weight = jnp.where(lane_task == wanted - b * chunk, weigh(raw), 0.0)
            total = total + jnp.sum(weight, axis=1, keepdims=True)
            mix = mix + dot(weight.astype(BF16), prompt_v[part, 1].reshape(keys, HD))
        span = heads * rows
        for i, s in enumerate(slots):
            prompt_mix[s] = mix[i * span : (i + 1) * span]
            prompt_total[s] = jnp.broadcast_to(total[i * span : (i + 1) * span], (span, HD))

    def arrive(route):
        came = source(*route)
        pltpu.make_async_remote_copy(
            src_ref=all_query.at[came],
            dst_ref=all_query.at[came],
            send_sem=q_send_sem,
            recv_sem=q_recv_sem.at[2 * route[0] + route[1]],
            device_id={"seq": came},
            device_id_type=MESH,
        ).wait_recv()
        return came

    bulk[1].wait()
    attend_prompts([me])

    small[4].wait()
    turned = table_v[...].astype(F32)
    page_id = (iota((pages, requests), 0) + me * pages).astype(F32)
    live = jnp.zeros((pages, requests), F32)
    for j in range(blocks):
        live = jnp.where(turned[j : j + 1, :] == page_id, length_row - float(j * block), live)
    owner = jnp.where(live > 0.0, 1.0, 0.0)
    valid = jnp.minimum(jnp.sum(live, axis=1, keepdims=True), float(block))
    owner_t = owner.T.astype(BF16)
    owner = owner.astype(BF16)

    far = farthest_first(chips)
    arrivals = [[(0, 1)], [(a, o) for a in far if a in (1, chips - 1) for o in (0, 1)]]
    rest = [(a, o) for a in far if a not in (1, chips - 1) for o in (0, 1)]
    if rest:
        arrivals.append(rest)
    for batch in arrivals:
        attend_prompts([arrive(route) for route in batch])
    queries = all_query[...].reshape(requests, heads * HD)

    page_query = dot(owner, queries)
    bulk[0].wait()
    group = 8
    span = group * block
    lane = iota((heads * group, span), 1)
    row = lax.rem(iota((heads * group, span), 0), group)
    own_page = lax.div(lane, block) == row
    token = lax.rem(lane, block).astype(F32)
    token = jnp.where(own_page, token, float(2 * block))
    for g in range(pages // group):
        part = slice(g * group, (g + 1) * group)
        left = jnp.concatenate(
            [page_query[part, h * HD : (h + 1) * HD] for h in range(heads)], axis=0
        ).astype(BF16)
        count = jnp.concatenate([valid[part]] * heads, axis=0)
        raw = dot(left, pool_v[part, 0].reshape(span, HD), NT)
        weight = jnp.where(token < count, weigh(raw), 0.0)
        total = jnp.sum(weight, axis=1, keepdims=True)
        mix = dot(weight.astype(BF16), pool_v[part, 1].reshape(span, HD))
        for h in range(heads):
            page_mix[part, h * HD : (h + 1) * HD] = mix[h * group : (h + 1) * group]
        high = total.astype(BF16).astype(F32)
        low = total - high
        fine = iota((group, HD), 1)
        columns = [x[h * group : (h + 1) * group] for h in range(heads) for x in (high, low)]
        page_mix[part, heads * HD :] = spread_lanes(columns, fine)
    spread = dot(owner_t, page_mix[...].astype(BF16))

    lanes = HD // (2 * heads)
    sums = []
    for h in range(heads):
        part = slice(h * rows, (h + 1) * rows)
        mix_send[:, part] = (
            spread[:, h * HD : (h + 1) * HD].reshape(seq, rows, HD) + prompt_mix[:, part]
        ).astype(BF16)
        at = heads * HD + 2 * h * lanes
        sums.append(
            spread[:, at : at + 1]
            + spread[:, at + lanes : at + lanes + 1]
            + prompt_total[:, part, :1].reshape(requests, 1)
        )
    fine = iota((8, HD), 1)
    for j in range(seq):
        columns = []
        for h in range(heads):
            for q in range(rows // 8):
                total = sums[h][j * rows + q * 8 : j * rows + q * 8 + 8]
                high = total.astype(BF16).astype(F32)
                columns += [high, total - high]
        mix_send[j, heads * rows :] = spread_lanes(columns, fine).astype(BF16)

    for ahead, other in routes:
        copy = pltpu.make_async_remote_copy(
            src_ref=mix_send.at[slot(ahead, other)],
            dst_ref=mix_recv.at[2 * ahead + other],
            send_sem=m_send_sem,
            recv_sem=m_recv_sem,
            device_id={"seq": slot(ahead, other)},
            device_id_type=MESH,
        )
        copy.start()
    whole = mix_send[me].astype(F32)
    bulk[2].wait()
    small[6].wait()
    arrived(mix_recv.at[pl.ds(1, seq - 1)], m_recv_sem)
    for d in range(1, seq):
        whole = whole + mix_recv[d].astype(F32)
    table = whole[heads * rows :]
    attended = []
    for h in range(heads):
        line = rows // 8
        lanes = HD // (2 * heads * line)
        total = jnp.concatenate(
            [
                table[:, (2 * q) * lanes : (2 * q) * lanes + 1]
                + table[:, (2 * q + 1) * lanes : (2 * q + 1) * lanes + 1]
                for q in range(h * line, (h + 1) * line)
            ],
            axis=0,
        )
        total = total + self_weight[h]
        mix = whole[h * rows : (h + 1) * rows] + self_mix[h]
        attended.append((mix / total).astype(BF16))
    projected = dot(jnp.concatenate(attended, axis=1), wo_v[...])

    tail = cols % HD
    full = cols // HD
    fold = HD // tail
    step = rows // fold
    for k in range(tensor):
        piece = projected[:, k * cols : (k + 1) * cols]
        for f in range(full):
            proj_send[k, f * rows : (f + 1) * rows] = piece[:, f * HD : (f + 1) * HD].astype(BF16)
        end = piece[:, full * HD :]
        proj_send[k, full * rows :] = jnp.concatenate(
            [end[i * step : (i + 1) * step] for i in range(fold)], axis=1
        ).astype(BF16)
    for d in farthest_first(tensor):

        @pl.when(place + d < tensor)
        def _(d=d):
            pl.semaphore_wait(here.at[place + d], 1)

        pltpu.make_async_remote_copy(
            src_ref=proj_send.at[tensor_peer(d)],
            dst_ref=proj_recv.at[d],
            send_sem=p_send_sem,
            recv_sem=p_recv_sem,
            device_id={"tensor": tensor_peer(d)},
            device_id_type=MESH,
        ).start()
    share = proj_send[mine].astype(F32)
    start = mine * cols
    base = lax.div(start, HD) * HD
    reach = (full + 1) * HD
    residual = hidden_v[:, pl.ds(pl.multiple_of(base, HD), reach)].astype(F32)
    residual = pltpu.roll(residual, lax.rem(reach - (start - base), reach), 1)
    arrived(proj_recv.at[pl.ds(1, tensor - 1)], p_recv_sem)
    for d in range(1, tensor):
        share = share + proj_recv[d].astype(F32)

    squares = share * share
    body_sum = squares[:rows]
    for f in range(1, full):
        body_sum = body_sum + squares[f * rows : (f + 1) * rows]
    body_sum = jnp.sum(body_sum, axis=1, keepdims=True)
    ends = squares[full * rows :]
    lane = iota((step, HD), 1)
    down = iota((step, HD), 0)
    line = jnp.zeros((step, HD), F32)
    for i in range(fold):
        of_end = jnp.sum(
            jnp.where(lax.div(lane, tail) == i, ends, 0.0), axis=1, keepdims=True
        )
        line = jnp.where(
            lane == i * tail + down, body_sum[i * step : (i + 1) * step] + of_end, line
        )
    square[0] = jnp.sum(line, axis=0, keepdims=True)
    for d in farthest_first(tensor):
        copy = pltpu.make_async_remote_copy(
            src_ref=square.at[0],
            dst_ref=square.at[d],
            send_sem=s_send_sem,
            recv_sem=s_recv_sem,
            device_id={"tensor": tensor_peer(d)},
            device_id_type=MESH,
        )
        copy.start()
    arrived(square.at[pl.ds(1, tensor - 1)], s_recv_sem)
    summed = square[0]
    for d in range(1, tensor):
        summed = summed + square[d]
    inverse = lax.rsqrt(summed * (1.0 / width) + EPS)
    columns = [
        jnp.sum(jnp.where(lane == i * tail + down, inverse, 0.0), axis=1, keepdims=True)
        for i in range(fold)
    ]
    post = post_v[...].reshape(1, -1)
    inverse = jnp.concatenate(columns, axis=0)
    for f in range(full):
        part = slice(f * HD, (f + 1) * HD)
        out_ref[:, part] = (
            residual[:, part] + share[f * rows : (f + 1) * rows] * inverse * post[:, part]
        ).astype(BF16)
    end = jnp.concatenate(
        [share[full * rows :, i * tail : (i + 1) * tail] for i in range(fold)], axis=0
    )
    out_ref[:, full * HD :] = (
        residual[:, full * HD : cols] + end * inverse * post[:, full * HD :]
    ).astype(BF16)

    arrived(all_query.at[pl.ds(0, seq - 1)], q_send_sem)
    arrived(mix_send.at[pl.ds(0, seq - 1)], m_send_sem)
    arrived(proj_send.at[pl.ds(0, tensor - 1)], p_send_sem)
    arrived(square.at[pl.ds(0, tensor - 1)], s_send_sem)


def hand_out(out_ref, fresh_ref, out, fresh):
    out[...] = out_ref[...]
    fresh[...] = fresh_ref[...]


def body(
    seq,
    tensor,
    hidden,
    pre_gain,
    w_query,
    w_key,
    w_value,
    w_out,
    post_gain,
    cache_pool,
    prompt_cache,
    task_ids,
    cache_lengths,
    block_table,
):
    rows, width = hidden.shape
    cols = post_gain.shape[0]
    heads = w_query.shape[1] // HD
    pages = cache_pool.shape[0]
    lines = rows * cols // HD
    pieces = 6
    half = HD // 2
    freq = np.float32(10000.0) ** (-np.arange(half, dtype=np.float64) / half)
    freq = jnp.asarray(np.concatenate([freq, freq])[None].astype(np.float32))
    args = (
        hidden,
        pre_gain,
        w_query,
        w_key,
        w_value,
        w_out,
        post_gain,
        cache_pool,
        prompt_cache,
        task_ids.reshape(1, -1),
        cache_lengths.reshape(1, -1),
        block_table.T,
        freq,
    )
    wide = (heads + 1) * HD
    dma = pltpu.SemaphoreType.DMA
    outs = pl.pallas_call(
        functools.partial(layer, seq=seq, tensor=tensor, pieces=pieces),
        out_shape=(
            pltpu.VMEM((rows, cols), BF16),
            pltpu.VMEM((rows, 2, HD), BF16),
        ),
        in_specs=[pl.BlockSpec(memory_space=pltpu.HBM)] * len(args),
        out_specs=[pl.BlockSpec(memory_space=pltpu.VMEM)] * 2,
        scratch_shapes=[pltpu.VMEM(a.shape, a.dtype) for a in args]
        + [
            pltpu.VMEM((pages, wide), F32),
            pltpu.VMEM((seq, heads * rows, HD), F32),
            pltpu.VMEM((seq, heads * rows, HD), F32),
            pltpu.VMEM((seq, rows, HD), jnp.int32),
            pltpu.VMEM((seq, rows, heads * HD), BF16),
            pltpu.VMEM((seq, heads * rows + 8, HD), BF16),
            pltpu.VMEM((seq, heads * rows + 8, HD), BF16),
            pltpu.VMEM((tensor, lines, HD), BF16),
            pltpu.VMEM((tensor, lines, HD), BF16),
            pltpu.VMEM((tensor, 1, HD), F32),
            pltpu.SemaphoreType.REGULAR((tensor,)),
            dma((10,)),
            dma((pieces,)),
            dma,
            dma((seq,)),
        ]
        + [dma] * 6,
        compiler_params=pltpu.CompilerParams(
            collective_id=0, has_side_effects=True, vmem_limit_bytes=60 * 1024 * 1024
        ),
        name="layer",
    )(*args)
    return pl.pallas_call(
        hand_out,
        out_shape=tuple(jax.ShapeDtypeStruct(a.shape, a.dtype) for a in outs),
        in_specs=[pl.BlockSpec(memory_space=pltpu.VMEM)] * 2,
        out_specs=[pl.BlockSpec(memory_space=pltpu.VMEM)] * 2,
        name="hand_out",
    )(*(pltpu.with_memory_space_constraint(a, pltpu.VMEM) for a in outs))


def solution(mesh):
    seq = mesh.shape["seq"]
    tensor = mesh.shape["tensor"]
    return jax.shard_map(
        functools.partial(body, seq, tensor),
        mesh=mesh,
        in_specs=(
            P(("groups", "seq"), None),
            P(),
            P(None, "tensor"),
            P(None, "tensor"),
            P(None, "tensor"),
            P("tensor", None),
            P("tensor"),
            P(("groups", "seq"), None, None, "tensor"),
            P("seq", None, None, "tensor"),
            P("groups"),
            P("groups"),
            P("groups", None),
        ),
        out_specs=(P(("groups", "seq"), "tensor"), P(("groups", "seq"), None, "tensor")),
        check_vma=False,
    )
```

```python
import functools
import math

import jax
import jax.numpy as jnp
import numpy as np
from jax import lax
from jax.experimental import pallas as pl
from jax.experimental.pallas import tpu as pltpu
from jax.sharding import PartitionSpec as P

D = 4608
H = 32
HD = 128
CAP = 50.0
EPS = 1e-6
MESH = pl.DeviceIdType.MESH
F32 = jnp.float32
BF16 = jnp.bfloat16
NT = (((1,), (1,)), ((), ()))
NN = (((1,), (0,)), ((), ()))

INNER = float(D // H) ** (-0.5) / CAP
OUTER = CAP * math.log2(math.e)


def dot(a, b, dims=NN):
    return lax.dot_general(a, b, dims, preferred_element_type=F32)


def weigh(raw):
    return jnp.exp2(OUTER * jnp.tanh(raw * INNER))


def iota(shape, dim):
    return lax.broadcasted_iota(jnp.int32, shape, dim)


def spread_lanes(columns, lane):
    width = lane.shape[1] // len(columns)
    out = jnp.broadcast_to(columns[0], lane.shape)
    for i in range(1, len(columns)):
        out = jnp.where(lane >= i * width, columns[i], out)
    return out


def farthest_first(size):
    return sorted(range(1, size), key=lambda d: -min(d, size - d))


def layer(
    hidden_hbm,
    gain_hbm,
    wq_hbm,
    wk_hbm,
    wv_hbm,
    wo_hbm,
    post_hbm,
    pool_hbm,
    prompt_hbm,
    task_hbm,
    length_hbm,
    table_hbm,
    freq_hbm,
    out_ref,
    fresh_ref,
    hidden_v,
    gain_v,
    wq_v,
    wk_v,
    wv_v,
    wo_v,
    post_v,
    pool_v,
    prompt_v,
    task_v,
    length_v,
    table_v,
    freq_v,
    page_mix,
    prompt_mix,
    prompt_total,
    task_column,
    all_query,
    mix_send,
    mix_recv,
    proj_send,
    proj_recv,
    square,
    here,
    in_sem,
    w_sem,
    q_send_sem,
    q_recv_sem,
    m_send_sem,
    m_recv_sem,
    p_send_sem,
    p_recv_sem,
    s_send_sem,
    s_recv_sem,
    *,
    seq,
    tensor,
    pieces,
):
    me = lax.axis_index("seq")
    mine = lax.axis_index("tensor")
    rows, width = hidden_v.shape
    requests = task_v.shape[1]
    pages = pool_v.shape[0]
    block = pool_v.shape[2]
    tasks, _, prompt, _ = prompt_v.shape
    blocks = table_v.shape[0]
    cols = out_ref.shape[1]

    chips = seq // 2
    chip, core = lax.div(me, 2), lax.rem(me, 2)
    slot = lambda ahead, other: lax.rem(chip + ahead, chips) * 2 + lax.rem(core + other, 2)
    source = lambda ahead, other: slot((chips - ahead) % chips, other)
    routes = [
        (ahead, other)
        for ahead in farthest_first(chips) + [0]
        for other in (1, 0)
        if ahead + other > 0
    ]
    tensor_peer = lambda d: lax.rem(mine + d, tensor)

    at_place = lambda p: (p + 1) % tensor
    place = lax.rem(mine + tensor - 1, tensor)

    def arrived(ref, sem):
        pltpu.make_async_copy(ref, ref, sem).wait()

    small = [
        pltpu.make_async_copy(src, dst, in_sem.at[i])
        for i, (src, dst) in enumerate(
            (
                (hidden_hbm, hidden_v),
                (gain_hbm, gain_v),
                (length_hbm, length_v),
                (freq_hbm, freq_v),
                (table_hbm, table_v),
                (task_hbm, task_v),
                (post_hbm, post_v),
            )
        )
    ]
    for copy in small:
        copy.start()
    depth = width // pieces
    weights = []
    for i in range(pieces):
        part = pl.ds(i * depth, depth)
        weights.append(
            [
                pltpu.make_async_copy(src.at[part], dst.at[part], w_sem.at[i])
                for src, dst in ((wq_hbm, wq_v), (wk_hbm, wk_v), (wv_hbm, wv_v))
            ]
        )
    for group in weights[: pieces // 2]:
        for copy in group:
            copy.start()
    bulk = [
        pltpu.make_async_copy(src, dst, in_sem.at[len(small) + i])
        for i, (src, dst) in enumerate(
            ((pool_hbm, pool_v), (prompt_hbm, prompt_v), (wo_hbm, wo_v))
        )
    ]

    barrier = pltpu.get_barrier_semaphore()
    for route in routes:
        pl.semaphore_signal(barrier, inc=1, device_id={"seq": slot(*route)}, device_id_type=MESH)
    for p in range(1, tensor):

        @pl.when(place < p)
        def _(p=p):
            pl.semaphore_signal(
                barrier, inc=1, device_id={"tensor": at_place(p)}, device_id_type=MESH
            )

    for copy in small[:4]:
        copy.wait()
    for group in weights[pieces // 2 :]:
        for copy in group:
            copy.start()

    values = hidden_v[...].astype(F32)
    scale = lax.rsqrt(jnp.mean(values * values, axis=-1, keepdims=True) + EPS)
    normed = (values * scale * gain_v[...].reshape(1, -1)).astype(BF16)

    length_row = length_v[...].astype(F32)
    at = iota((rows, requests), 0) + me * rows
    own_length = jnp.sum(
        jnp.where(at == iota((rows, requests), 1), length_row, 0.0), axis=1, keepdims=True
    )
    angles = (own_length + float(prompt)) * freq_v[...]
    cosine = jnp.cos(angles)
    sine = jnp.sin(angles)
    half = HD // 2
    sine = jnp.where(iota(sine.shape, 1) < half, -sine, sine)

    small[5].wait()
    same = iota((requests, requests), 0) == iota((requests, requests), 1)
    task = jnp.sum(
        jnp.where(same, task_v[...].astype(F32), 0.0), axis=1, keepdims=True
    ).astype(jnp.int32) - me * tasks
    task_column[...] = jnp.broadcast_to(task, (requests, HD)).reshape(seq, rows, HD)

    small[4].wait()
    turned = table_v[...].astype(F32)
    page_id = (iota((pages, requests), 0) + me * pages).astype(F32)
    live = jnp.zeros((pages, requests), F32)
    for j in range(blocks):
        live = jnp.where(turned[j : j + 1, :] == page_id, length_row - float(j * block), live)
    owner = jnp.where(live > 0.0, 1.0, 0.0)
    valid = jnp.minimum(jnp.sum(live, axis=1, keepdims=True), float(block))
    owner_t = owner.T.astype(BF16)
    owner = owner.astype(BF16)

    heads = wq_v.shape[1] // HD
    query = jnp.zeros((rows, wq_v.shape[1]), F32)
    key = jnp.zeros((rows, HD), F32)
    value = jnp.zeros((rows, HD), F32)
    for i in range(pieces):
        arrived(wq_v.at[pl.ds(0, 2 * depth)], w_sem.at[i])
        if i == pieces // 2:
            bulk[1].start()
        if i == pieces - 1:
            bulk[0].start()
            bulk[2].start()
        part = slice(i * depth, (i + 1) * depth)
        left = normed[:, part]
        query = query + dot(left, wq_v[part])
        key = key + dot(left, wk_v[part])
        value = value + dot(left, wv_v[part])

    def rope(x):
        return (x * cosine + pltpu.roll(x, half, 1) * sine).astype(BF16)

    own_query = [rope(query[:, h * HD : (h + 1) * HD]) for h in range(heads)]
    new_key = rope(key)
    new_value = value.astype(BF16)
    all_query[me] = jnp.concatenate(own_query, axis=1)

    pl.semaphore_wait(barrier, seq - 1 + place)
    q_copies = {}
    for ahead, other in routes:
        q_copies[ahead, other] = pltpu.make_async_remote_copy(
            src_ref=all_query.at[me],
            dst_ref=all_query.at[me],
            send_sem=q_send_sem,
            recv_sem=q_recv_sem.at[2 * ahead + other],
            device_id={"seq": slot(ahead, other)},
            device_id_type=MESH,
        )
        q_copies[ahead, other].start()

    for p in range(tensor - 1):

        @pl.when(p < place)
        def _(p=p):
            pl.semaphore_signal(
                here.at[place], inc=1, device_id={"tensor": at_place(p)}, device_id_type=MESH
            )

    fresh_ref[:, 0, :] = new_key
    fresh_ref[:, 1, :] = new_value

    key32 = new_key.astype(F32)
    value32 = new_value.astype(F32)
    self_weight = [
        weigh(jnp.sum(q.astype(F32) * key32, axis=1, keepdims=True)) for q in own_query
    ]
    self_mix = [w.astype(BF16).astype(F32) * value32 for w in self_weight]

    chunk = 8
    keys = chunk * prompt

    def attend_prompts(slots):
        left = jnp.concatenate(
            [all_query[s, :, h * HD : (h + 1) * HD] for s in slots for h in range(heads)], axis=0
        )
        wanted = jnp.concatenate(
            [task_column[s, :, :1] for s in slots for h in range(heads)], axis=0
        )
        count = left.shape[0]
        lane_task = lax.div(iota((count, keys), 1), prompt)
        total = jnp.zeros((count, 1), F32)
        mix = jnp.zeros((count, HD), F32)
        for b in range(tasks // chunk):
            part = slice(b * chunk, (b + 1) * chunk)
            raw = dot(left, prompt_v[part, 0].reshape(keys, HD), NT)
            weight = jnp.where(lane_task == wanted - b * chunk, weigh(raw), 0.0)
            total = total + jnp.sum(weight, axis=1, keepdims=True)
            mix = mix + dot(weight.astype(BF16), prompt_v[part, 1].reshape(keys, HD))
        span = heads * rows
        for i, s in enumerate(slots):
            prompt_mix[s] = mix[i * span : (i + 1) * span]
            prompt_total[s] = jnp.broadcast_to(total[i * span : (i + 1) * span], (span, HD))

    def arrive(route):
        came = source(*route)
        pltpu.make_async_remote_copy(
            src_ref=all_query.at[came],
            dst_ref=all_query.at[came],
            send_sem=q_send_sem,
            recv_sem=q_recv_sem.at[2 * route[0] + route[1]],
            device_id={"seq": came},
            device_id_type=MESH,
        ).wait_recv()
        return came

    bulk[1].wait()
    attend_prompts([me])

    far = farthest_first(chips)
    arrivals = [[(0, 1)], [(a, o) for a in far if a in (1, chips - 1) for o in (0, 1)]]
    rest = [(a, o) for a in far if a not in (1, chips - 1) for o in (0, 1)]
    if rest:
        arrivals.append(rest)
    for batch in arrivals:
        attend_prompts([arrive(route) for route in batch])
    queries = all_query[...].reshape(requests, heads * HD)

    page_query = dot(owner, queries)
    bulk[0].wait()
    group = 8
    span = group * block
    lane = iota((heads * group, span), 1)
    row = lax.rem(iota((heads * group, span), 0), group)
    own_page = lax.div(lane, block) == row
    token = lax.rem(lane, block).astype(F32)
    token = jnp.where(own_page, token, float(2 * block))
    for g in range(pages // group):
        part = slice(g * group, (g + 1) * group)
        left = jnp.concatenate(
            [page_query[part, h * HD : (h + 1) * HD] for h in range(heads)], axis=0
        ).astype(BF16)
        count = jnp.concatenate([valid[part]] * heads, axis=0)
        raw = dot(left, pool_v[part, 0].reshape(span, HD), NT)
        weight = jnp.where(token < count, weigh(raw), 0.0)
        total = jnp.sum(weight, axis=1, keepdims=True)
        mix = dot(weight.astype(BF16), pool_v[part, 1].reshape(span, HD))
        for h in range(heads):
            page_mix[part, h * HD : (h + 1) * HD] = mix[h * group : (h + 1) * group]
        high = total.astype(BF16).astype(F32)
        low = total - high
        fine = iota((group, HD), 1)
        columns = [x[h * group : (h + 1) * group] for h in range(heads) for x in (high, low)]
        page_mix[part, heads * HD :] = spread_lanes(columns, fine)
    spread = dot(owner_t, page_mix[...].astype(BF16))

    lanes = HD // (2 * heads)
    sums = []
    for h in range(heads):
        part = slice(h * rows, (h + 1) * rows)
        mix_send[:, part] = (
            spread[:, h * HD : (h + 1) * HD].reshape(seq, rows, HD) + prompt_mix[:, part]
        ).astype(BF16)
        at = heads * HD + 2 * h * lanes
        sums.append(
            spread[:, at : at + 1]
            + spread[:, at + lanes : at + lanes + 1]
            + prompt_total[:, part, :1].reshape(requests, 1)
        )
    fine = iota((8, HD), 1)
    for j in range(seq):
        columns = []
        for h in range(heads):
            for q in range(rows // 8):
                total = sums[h][j * rows + q * 8 : j * rows + q * 8 + 8]
                high = total.astype(BF16).astype(F32)
                columns += [high, total - high]
        mix_send[j, heads * rows :] = spread_lanes(columns, fine).astype(BF16)

    for ahead, other in routes:
        copy = pltpu.make_async_remote_copy(
            src_ref=mix_send.at[slot(ahead, other)],
            dst_ref=mix_recv.at[2 * ahead + other],
            send_sem=m_send_sem,
            recv_sem=m_recv_sem,
            device_id={"seq": slot(ahead, other)},
            device_id_type=MESH,
        )
        copy.start()
    whole = mix_send[me].astype(F32)
    bulk[2].wait()
    small[6].wait()
    arrived(mix_recv.at[pl.ds(1, seq - 1)], m_recv_sem)
    for d in range(1, seq):
        whole = whole + mix_recv[d].astype(F32)
    table = whole[heads * rows :]
    attended = []
    for h in range(heads):
        line = rows // 8
        lanes = HD // (2 * heads * line)
        total = jnp.concatenate(
            [
                table[:, (2 * q) * lanes : (2 * q) * lanes + 1]
                + table[:, (2 * q + 1) * lanes : (2 * q + 1) * lanes + 1]
                for q in range(h * line, (h + 1) * line)
            ],
            axis=0,
        )
        total = total + self_weight[h]
        mix = whole[h * rows : (h + 1) * rows] + self_mix[h]
        attended.append((mix / total).astype(BF16))
    projected = dot(jnp.concatenate(attended, axis=1), wo_v[...])

    tail = cols % HD
    full = cols // HD
    fold = HD // tail
    step = rows // fold
    for k in range(tensor):
        piece = projected[:, k * cols : (k + 1) * cols]
        for f in range(full):
            proj_send[k, f * rows : (f + 1) * rows] = piece[:, f * HD : (f + 1) * HD].astype(BF16)
        end = piece[:, full * HD :]
        proj_send[k, full * rows :] = jnp.concatenate(
            [end[i * step : (i + 1) * step] for i in range(fold)], axis=1
        ).astype(BF16)
    for d in farthest_first(tensor):

        @pl.when(place + d < tensor)
        def _(d=d):
            pl.semaphore_wait(here.at[place + d], 1)

        pltpu.make_async_remote_copy(
            src_ref=proj_send.at[tensor_peer(d)],
            dst_ref=proj_recv.at[d],
            send_sem=p_send_sem,
            recv_sem=p_recv_sem,
            device_id={"tensor": tensor_peer(d)},
            device_id_type=MESH,
        ).start()
    share = proj_send[mine].astype(F32)
    start = mine * cols
    base = lax.div(start, HD) * HD
    reach = (full + 1) * HD
    residual = hidden_v[:, pl.ds(pl.multiple_of(base, HD), reach)].astype(F32)
    residual = pltpu.roll(residual, lax.rem(reach - (start - base), reach), 1)
    arrived(proj_recv.at[pl.ds(1, tensor - 1)], p_recv_sem)
    for d in range(1, tensor):
        share = share + proj_recv[d].astype(F32)

    squares = share * share
    body_sum = squares[:rows]
    for f in range(1, full):
        body_sum = body_sum + squares[f * rows : (f + 1) * rows]
    body_sum = jnp.sum(body_sum, axis=1, keepdims=True)
    ends = squares[full * rows :]
    lane = iota((step, HD), 1)
    down = iota((step, HD), 0)
    line = jnp.zeros((step, HD), F32)
    for i in range(fold):
        of_end = jnp.sum(
            jnp.where(lax.div(lane, tail) == i, ends, 0.0), axis=1, keepdims=True
        )
        line = jnp.where(
            lane == i * tail + down, body_sum[i * step : (i + 1) * step] + of_end, line
        )
    square[0] = jnp.sum(line, axis=0, keepdims=True)
    for d in farthest_first(tensor):
        copy = pltpu.make_async_remote_copy(
            src_ref=square.at[0],
            dst_ref=square.at[d],
            send_sem=s_send_sem,
            recv_sem=s_recv_sem,
            device_id={"tensor": tensor_peer(d)},
            device_id_type=MESH,
        )
        copy.start()
    arrived(square.at[pl.ds(1, tensor - 1)], s_recv_sem)
    summed = square[0]
    for d in range(1, tensor):
        summed = summed + square[d]
    inverse = lax.rsqrt(summed * (1.0 / width) + EPS)
    columns = [
        jnp.sum(jnp.where(lane == i * tail + down, inverse, 0.0), axis=1, keepdims=True)
        for i in range(fold)
    ]
    post = post_v[...].reshape(1, -1)
    inverse = jnp.concatenate(columns, axis=0)
    for f in range(full):
        part = slice(f * HD, (f + 1) * HD)
        out_ref[:, part] = (
            residual[:, part] + share[f * rows : (f + 1) * rows] * inverse * post[:, part]
        ).astype(BF16)
    end = jnp.concatenate(
        [share[full * rows :, i * tail : (i + 1) * tail] for i in range(fold)], axis=0
    )
    out_ref[:, full * HD :] = (
        residual[:, full * HD : cols] + end * inverse * post[:, full * HD :]
    ).astype(BF16)

    arrived(all_query.at[pl.ds(0, seq - 1)], q_send_sem)
    arrived(mix_send.at[pl.ds(0, seq - 1)], m_send_sem)
    arrived(proj_send.at[pl.ds(0, tensor - 1)], p_send_sem)
    arrived(square.at[pl.ds(0, tensor - 1)], s_send_sem)


def hand_out(out_ref, fresh_ref, out, fresh):
    out[...] = out_ref[...]
    fresh[...] = fresh_ref[...]


def body(
    seq,
    tensor,
    hidden,
    pre_gain,
    w_query,
    w_key,
    w_value,
    w_out,
    post_gain,
    cache_pool,
    prompt_cache,
    task_ids,
    cache_lengths,
    block_table,
):
    rows, width = hidden.shape
    cols = post_gain.shape[0]
    heads = w_query.shape[1] // HD
    pages = cache_pool.shape[0]
    lines = rows * cols // HD
    pieces = 6
    half = HD // 2
    freq = np.float32(10000.0) ** (-np.arange(half, dtype=np.float64) / half)
    freq = jnp.asarray(np.concatenate([freq, freq])[None].astype(np.float32))
    args = (
        hidden,
        pre_gain,
        w_query,
        w_key,
        w_value,
        w_out,
        post_gain,
        cache_pool,
        prompt_cache,
        task_ids.reshape(1, -1),
        cache_lengths.reshape(1, -1),
        block_table.T,
        freq,
    )
    wide = (heads + 1) * HD
    dma = pltpu.SemaphoreType.DMA
    outs = pl.pallas_call(
        functools.partial(layer, seq=seq, tensor=tensor, pieces=pieces),
        out_shape=(
            pltpu.VMEM((rows, cols), BF16),
            pltpu.VMEM((rows, 2, HD), BF16),
        ),
        in_specs=[pl.BlockSpec(memory_space=pltpu.HBM)] * len(args),
        out_specs=[pl.BlockSpec(memory_space=pltpu.VMEM)] * 2,
        scratch_shapes=[pltpu.VMEM(a.shape, a.dtype) for a in args]
        + [
            pltpu.VMEM((pages, wide), F32),
            pltpu.VMEM((seq, heads * rows, HD), F32),
            pltpu.VMEM((seq, heads * rows, HD), F32),
            pltpu.VMEM((seq, rows, HD), jnp.int32),
            pltpu.VMEM((seq, rows, heads * HD), BF16),
            pltpu.VMEM((seq, heads * rows + 8, HD), BF16),
            pltpu.VMEM((seq, heads * rows + 8, HD), BF16),
            pltpu.VMEM((tensor, lines, HD), BF16),
            pltpu.VMEM((tensor, lines, HD), BF16),
            pltpu.VMEM((tensor, 1, HD), F32),
            pltpu.SemaphoreType.REGULAR((tensor,)),
            dma((10,)),
            dma((pieces,)),
            dma,
            dma((seq,)),
        ]
        + [dma] * 6,
        compiler_params=pltpu.CompilerParams(
            collective_id=0, has_side_effects=True, vmem_limit_bytes=60 * 1024 * 1024
        ),
        name="layer",
    )(*args)
    return pl.pallas_call(
        hand_out,
        out_shape=tuple(jax.ShapeDtypeStruct(a.shape, a.dtype) for a in outs),
        in_specs=[pl.BlockSpec(memory_space=pltpu.VMEM)] * 2,
        out_specs=[pl.BlockSpec(memory_space=pltpu.VMEM)] * 2,
        name="hand_out",
    )(*(pltpu.with_memory_space_constraint(a, pltpu.VMEM) for a in outs))


def solution(mesh):
    seq = mesh.shape["seq"]
    tensor = mesh.shape["tensor"]
    return jax.shard_map(
        functools.partial(body, seq, tensor),
        mesh=mesh,
        in_specs=(
            P(("groups", "seq"), None),
            P(),
            P(None, "tensor"),
            P(None, "tensor"),
            P(None, "tensor"),
            P("tensor", None),
            P("tensor"),
            P(("groups", "seq"), None, None, "tensor"),
            P("seq", None, None, "tensor"),
            P("groups"),
            P("groups"),
            P("groups", None),
        ),
        out_specs=(P(("groups", "seq"), "tensor"), P(("groups", "seq"), None, "tensor")),
        check_vma=False,
    )
```

```python
import functools
import math

import jax
import jax.numpy as jnp
import numpy as np
from jax import lax
from jax.experimental import pallas as pl
from jax.experimental.pallas import tpu as pltpu
from jax.sharding import PartitionSpec as P

D = 4608
H = 32
HD = 128
CAP = 50.0
EPS = 1e-6
MESH = pl.DeviceIdType.MESH
F32 = jnp.float32
BF16 = jnp.bfloat16
NT = (((1,), (1,)), ((), ()))
NN = (((1,), (0,)), ((), ()))

INNER = float(D // H) ** (-0.5) / CAP
OUTER = CAP * math.log2(math.e)


def dot(a, b, dims=NN):
    return lax.dot_general(a, b, dims, preferred_element_type=F32)


def weigh(raw):
    return jnp.exp2(OUTER * jnp.tanh(raw * INNER))


def iota(shape, dim):
    return lax.broadcasted_iota(jnp.int32, shape, dim)


def spread_lanes(columns, lane):
    width = lane.shape[1] // len(columns)
    out = jnp.broadcast_to(columns[0], lane.shape)
    for i in range(1, len(columns)):
        out = jnp.where(lane >= i * width, columns[i], out)
    return out


def farthest_first(size):
    return sorted(range(1, size), key=lambda d: -min(d, size - d))


def layer(
    hidden_hbm,
    gain_hbm,
    wq_hbm,
    wk_hbm,
    wv_hbm,
    wo_hbm,
    post_hbm,
    pool_hbm,
    prompt_hbm,
    task_hbm,
    length_hbm,
    table_hbm,
    freq_hbm,
    out_ref,
    fresh_ref,
    hidden_v,
    gain_v,
    wq_v,
    wk_v,
    wv_v,
    wo_v,
    post_v,
    pool_v,
    prompt_v,
    task_v,
    length_v,
    table_v,
    freq_v,
    page_mix,
    prompt_mix,
    prompt_total,
    task_column,
    all_query,
    mix_send,
    mix_recv,
    proj_send,
    proj_recv,
    square,
    here,
    in_sem,
    w_sem,
    q_send_sem,
    q_recv_sem,
    m_send_sem,
    m_recv_sem,
    p_send_sem,
    p_recv_sem,
    s_send_sem,
    s_recv_sem,
    *,
    seq,
    tensor,
    pieces,
):
    me = lax.axis_index("seq")
    mine = lax.axis_index("tensor")
    rows, width = hidden_v.shape
    requests = task_v.shape[1]
    pages = pool_v.shape[0]
    block = pool_v.shape[2]
    tasks, _, prompt, _ = prompt_v.shape
    blocks = table_v.shape[0]
    cols = out_ref.shape[1]

    chips = seq // 2
    chip, core = lax.div(me, 2), lax.rem(me, 2)
    slot = lambda ahead, other: lax.rem(chip + ahead, chips) * 2 + lax.rem(core + other, 2)
    source = lambda ahead, other: slot((chips - ahead) % chips, other)
    routes = [
        (ahead, other)
        for ahead in farthest_first(chips) + [0]
        for other in (1, 0)
        if ahead + other > 0
    ]
    tensor_peer = lambda d: lax.rem(mine + d, tensor)

    at_place = lambda p: (p + 1) % tensor
    place = lax.rem(mine + tensor - 1, tensor)

    def arrived(ref, sem):
        pltpu.make_async_copy(ref, ref, sem).wait()

    small = [
        pltpu.make_async_copy(src, dst, in_sem.at[i])
        for i, (src, dst) in enumerate(
            (
                (hidden_hbm, hidden_v),
                (gain_hbm, gain_v),
                (length_hbm, length_v),
                (freq_hbm, freq_v),
                (table_hbm, table_v),
                (task_hbm, task_v),
                (post_hbm, post_v),
            )
        )
    ]
    for copy in small:
        copy.start()
    depth = width // pieces
    weights = []
    for i in range(pieces):
        part = pl.ds(i * depth, depth)
        weights.append(
            [
                pltpu.make_async_copy(src.at[part], dst.at[part], w_sem.at[i])
                for src, dst in ((wq_hbm, wq_v), (wk_hbm, wk_v), (wv_hbm, wv_v))
            ]
        )
    for group in weights[: pieces // 2]:
        for copy in group:
            copy.start()
    bulk = [
        pltpu.make_async_copy(src, dst, in_sem.at[len(small) + i])
        for i, (src, dst) in enumerate(
            ((pool_hbm, pool_v), (prompt_hbm, prompt_v), (wo_hbm, wo_v))
        )
    ]

    barrier = pltpu.get_barrier_semaphore()
    for route in routes:
        pl.semaphore_signal(barrier, inc=1, device_id={"seq": slot(*route)}, device_id_type=MESH)
    for p in range(1, tensor):

        @pl.when(place < p)
        def _(p=p):
            pl.semaphore_signal(
                barrier, inc=1, device_id={"tensor": at_place(p)}, device_id_type=MESH
            )

    for copy in small[:4]:
        copy.wait()
    for group in weights[pieces // 2 :]:
        for copy in group:
            copy.start()

    values = hidden_v[...].astype(F32)
    scale = lax.rsqrt(jnp.mean(values * values, axis=-1, keepdims=True) + EPS)
    normed = (values * scale * gain_v[...].reshape(1, -1)).astype(BF16)

    length_row = length_v[...].astype(F32)
    at = iota((rows, requests), 0) + me * rows
    own_length = jnp.sum(
        jnp.where(at == iota((rows, requests), 1), length_row, 0.0), axis=1, keepdims=True
    )
    angles = (own_length + float(prompt)) * freq_v[...]
    cosine = jnp.cos(angles)
    sine = jnp.sin(angles)
    half = HD // 2
    sine = jnp.where(iota(sine.shape, 1) < half, -sine, sine)

    small[5].wait()
    same = iota((requests, requests), 0) == iota((requests, requests), 1)
    task = jnp.sum(
        jnp.where(same, task_v[...].astype(F32), 0.0), axis=1, keepdims=True
    ).astype(jnp.int32) - me * tasks
    task_column[...] = jnp.broadcast_to(task, (requests, HD)).reshape(seq, rows, HD)

    small[4].wait()
    turned = table_v[...].astype(F32)
    page_id = (iota((pages, requests), 0) + me * pages).astype(F32)
    live = jnp.zeros((pages, requests), F32)
    for j in range(blocks):
        live = jnp.where(turned[j : j + 1, :] == page_id, length_row - float(j * block), live)
    owner = jnp.where(live > 0.0, 1.0, 0.0)
    valid = jnp.minimum(jnp.sum(live, axis=1, keepdims=True), float(block))
    owner_t = owner.T.astype(BF16)
    owner = owner.astype(BF16)

    heads = wq_v.shape[1] // HD
    query = jnp.zeros((rows, wq_v.shape[1]), F32)
    key = jnp.zeros((rows, HD), F32)
    value = jnp.zeros((rows, HD), F32)
    for i in range(pieces):
        arrived(wq_v.at[pl.ds(0, 2 * depth)], w_sem.at[i])
        if i == pieces // 2:
            bulk[1].start()
        if i == pieces - 1:
            bulk[0].start()
            bulk[2].start()
        part = slice(i * depth, (i + 1) * depth)
        left = normed[:, part]
        query = query + dot(left, wq_v[part])
        key = key + dot(left, wk_v[part])
        value = value + dot(left, wv_v[part])

    def rope(x):
        return (x * cosine + pltpu.roll(x, half, 1) * sine).astype(BF16)

    own_query = [rope(query[:, h * HD : (h + 1) * HD]) for h in range(heads)]
    new_key = rope(key)
    new_value = value.astype(BF16)
    all_query[me] = jnp.concatenate(own_query, axis=1)

    pl.semaphore_wait(barrier, seq - 1 + place)
    q_copies = {}
    for ahead, other in routes:
        q_copies[ahead, other] = pltpu.make_async_remote_copy(
            src_ref=all_query.at[me],
            dst_ref=all_query.at[me],
            send_sem=q_send_sem,
            recv_sem=q_recv_sem.at[2 * ahead + other],
            device_id={"seq": slot(ahead, other)},
            device_id_type=MESH,
        )
        q_copies[ahead, other].start()

    for p in range(tensor - 1):

        @pl.when(p < place)
        def _(p=p):
            pl.semaphore_signal(
                here.at[place], inc=1, device_id={"tensor": at_place(p)}, device_id_type=MESH
            )

    fresh_ref[:, 0, :] = new_key
    fresh_ref[:, 1, :] = new_value

    key32 = new_key.astype(F32)
    value32 = new_value.astype(F32)
    self_weight = [
        weigh(jnp.sum(q.astype(F32) * key32, axis=1, keepdims=True)) for q in own_query
    ]
    self_mix = [w.astype(BF16).astype(F32) * value32 for w in self_weight]


    def attend_prompts(slots):
        left = jnp.concatenate(
            [all_query[s, :, h * HD : (h + 1) * HD] for s in slots for h in range(heads)], axis=0
        )
        wanted = jnp.concatenate(
            [task_column[s, :, :1] for s in slots for h in range(heads)], axis=0
        )
        count = left.shape[0]
        chunk = tasks
        keys = chunk * prompt
        lane_task = lax.div(iota((count, keys), 1), prompt)
        total = jnp.zeros((count, 1), F32)
        mix = jnp.zeros((count, HD), F32)
        for b in range(tasks // chunk):
            part = slice(b * chunk, (b + 1) * chunk)
            raw = dot(left, prompt_v[part, 0].reshape(keys, HD), NT)
            weight = jnp.where(lane_task == wanted - b * chunk, weigh(raw), 0.0)
            total = total + jnp.sum(weight, axis=1, keepdims=True)
            mix = mix + dot(weight.astype(BF16), prompt_v[part, 1].reshape(keys, HD))
        span = heads * rows
        for i, s in enumerate(slots):
            prompt_mix[s] = mix[i * span : (i + 1) * span]
            prompt_total[s] = jnp.broadcast_to(total[i * span : (i + 1) * span], (span, HD))

    def arrive(route):
        came = source(*route)
        pltpu.make_async_remote_copy(
            src_ref=all_query.at[came],
            dst_ref=all_query.at[came],
            send_sem=q_send_sem,
            recv_sem=q_recv_sem.at[2 * route[0] + route[1]],
            device_id={"seq": came},
            device_id_type=MESH,
        ).wait_recv()
        return came

    bulk[1].wait()
    attend_prompts([me])

    far = farthest_first(chips)
    arrivals = [[(0, 1)], [(a, o) for a in far if a in (1, chips - 1) for o in (0, 1)]]
    rest = [(a, o) for a in far if a not in (1, chips - 1) for o in (0, 1)]
    if rest:
        arrivals.append(rest)
    for batch in arrivals:
        attend_prompts([arrive(route) for route in batch])
    queries = all_query[...].reshape(requests, heads * HD)

    page_query = dot(owner, queries)
    bulk[0].wait()
    group = 8
    span = group * block
    lane = iota((heads * group, span), 1)
    row = lax.rem(iota((heads * group, span), 0), group)
    own_page = lax.div(lane, block) == row
    token = lax.rem(lane, block).astype(F32)
    token = jnp.where(own_page, token, float(2 * block))
    for g in range(pages // group):
        part = slice(g * group, (g + 1) * group)
        left = jnp.concatenate(
            [page_query[part, h * HD : (h + 1) * HD] for h in range(heads)], axis=0
        ).astype(BF16)
        count = jnp.concatenate([valid[part]] * heads, axis=0)
        raw = dot(left, pool_v[part, 0].reshape(span, HD), NT)
        weight = jnp.where(token < count, weigh(raw), 0.0)
        total = jnp.sum(weight, axis=1, keepdims=True)
        mix = dot(weight.astype(BF16), pool_v[part, 1].reshape(span, HD))
        for h in range(heads):
            page_mix[part, h * HD : (h + 1) * HD] = mix[h * group : (h + 1) * group]
        high = total.astype(BF16).astype(F32)
        low = total - high
        fine = iota((group, HD), 1)
        columns = [x[h * group : (h + 1) * group] for h in range(heads) for x in (high, low)]
        page_mix[part, heads * HD :] = spread_lanes(columns, fine)
    spread = dot(owner_t, page_mix[...].astype(BF16))

    lanes = HD // (2 * heads)
    sums = []
    for h in range(heads):
        part = slice(h * rows, (h + 1) * rows)
        mix_send[:, part] = (
            spread[:, h * HD : (h + 1) * HD].reshape(seq, rows, HD) + prompt_mix[:, part]
        ).astype(BF16)
        at = heads * HD + 2 * h * lanes
        sums.append(
            spread[:, at : at + 1]
            + spread[:, at + lanes : at + lanes + 1]
            + prompt_total[:, part, :1].reshape(requests, 1)
        )
    fine = iota((8, HD), 1)
    for j in range(seq):
        columns = []
        for h in range(heads):
            for q in range(rows // 8):
                total = sums[h][j * rows + q * 8 : j * rows + q * 8 + 8]
                high = total.astype(BF16).astype(F32)
                columns += [high, total - high]
        mix_send[j, heads * rows :] = spread_lanes(columns, fine).astype(BF16)

    for ahead, other in routes:
        copy = pltpu.make_async_remote_copy(
            src_ref=mix_send.at[slot(ahead, other)],
            dst_ref=mix_recv.at[2 * ahead + other],
            send_sem=m_send_sem,
            recv_sem=m_recv_sem,
            device_id={"seq": slot(ahead, other)},
            device_id_type=MESH,
        )
        copy.start()
    whole = mix_send[me].astype(F32)
    bulk[2].wait()
    small[6].wait()
    arrived(mix_recv.at[pl.ds(1, seq - 1)], m_recv_sem)
    for d in range(1, seq):
        whole = whole + mix_recv[d].astype(F32)
    table = whole[heads * rows :]
    attended = []
    for h in range(heads):
        line = rows // 8
        lanes = HD // (2 * heads * line)
        total = jnp.concatenate(
            [
                table[:, (2 * q) * lanes : (2 * q) * lanes + 1]
                + table[:, (2 * q + 1) * lanes : (2 * q + 1) * lanes + 1]
                for q in range(h * line, (h + 1) * line)
            ],
            axis=0,
        )
        total = total + self_weight[h]
        mix = whole[h * rows : (h + 1) * rows] + self_mix[h]
        attended.append((mix / total).astype(BF16))
    projected = dot(jnp.concatenate(attended, axis=1), wo_v[...])

    tail = cols % HD
    full = cols // HD
    fold = HD // tail
    step = rows // fold
    for k in range(tensor):
        piece = projected[:, k * cols : (k + 1) * cols]
        for f in range(full):
            proj_send[k, f * rows : (f + 1) * rows] = piece[:, f * HD : (f + 1) * HD].astype(BF16)
        end = piece[:, full * HD :]
        proj_send[k, full * rows :] = jnp.concatenate(
            [end[i * step : (i + 1) * step] for i in range(fold)], axis=1
        ).astype(BF16)
    for d in farthest_first(tensor):

        @pl.when(place + d < tensor)
        def _(d=d):
            pl.semaphore_wait(here.at[place + d], 1)

        pltpu.make_async_remote_copy(
            src_ref=proj_send.at[tensor_peer(d)],
            dst_ref=proj_recv.at[d],
            send_sem=p_send_sem,
            recv_sem=p_recv_sem,
            device_id={"tensor": tensor_peer(d)},
            device_id_type=MESH,
        ).start()
    share = proj_send[mine].astype(F32)
    start = mine * cols
    base = lax.div(start, HD) * HD
    reach = (full + 1) * HD
    residual = hidden_v[:, pl.ds(pl.multiple_of(base, HD), reach)].astype(F32)
    residual = pltpu.roll(residual, lax.rem(reach - (start - base), reach), 1)
    arrived(proj_recv.at[pl.ds(1, tensor - 1)], p_recv_sem)
    for d in range(1, tensor):
        share = share + proj_recv[d].astype(F32)

    squares = share * share
    body_sum = squares[:rows]
    for f in range(1, full):
        body_sum = body_sum + squares[f * rows : (f + 1) * rows]
    body_sum = jnp.sum(body_sum, axis=1, keepdims=True)
    ends = squares[full * rows :]
    lane = iota((step, HD), 1)
    down = iota((step, HD), 0)
    line = jnp.zeros((step, HD), F32)
    for i in range(fold):
        of_end = jnp.sum(
            jnp.where(lax.div(lane, tail) == i, ends, 0.0), axis=1, keepdims=True
        )
        line = jnp.where(
            lane == i * tail + down, body_sum[i * step : (i + 1) * step] + of_end, line
        )
    square[0] = jnp.sum(line, axis=0, keepdims=True)
    for d in farthest_first(tensor):
        copy = pltpu.make_async_remote_copy(
            src_ref=square.at[0],
            dst_ref=square.at[d],
            send_sem=s_send_sem,
            recv_sem=s_recv_sem,
            device_id={"tensor": tensor_peer(d)},
            device_id_type=MESH,
        )
        copy.start()
    arrived(square.at[pl.ds(1, tensor - 1)], s_recv_sem)
    summed = square[0]
    for d in range(1, tensor):
        summed = summed + square[d]
    inverse = lax.rsqrt(summed * (1.0 / width) + EPS)
    columns = [
        jnp.sum(jnp.where(lane == i * tail + down, inverse, 0.0), axis=1, keepdims=True)
        for i in range(fold)
    ]
    post = post_v[...].reshape(1, -1)
    inverse = jnp.concatenate(columns, axis=0)
    for f in range(full):
        part = slice(f * HD, (f + 1) * HD)
        out_ref[:, part] = (
            residual[:, part] + share[f * rows : (f + 1) * rows] * inverse * post[:, part]
        ).astype(BF16)
    end = jnp.concatenate(
        [share[full * rows :, i * tail : (i + 1) * tail] for i in range(fold)], axis=0
    )
    out_ref[:, full * HD :] = (
        residual[:, full * HD : cols] + end * inverse * post[:, full * HD :]
    ).astype(BF16)

    arrived(all_query.at[pl.ds(0, seq - 1)], q_send_sem)
    arrived(mix_send.at[pl.ds(0, seq - 1)], m_send_sem)
    arrived(proj_send.at[pl.ds(0, tensor - 1)], p_send_sem)
    arrived(square.at[pl.ds(0, tensor - 1)], s_send_sem)


def hand_out(out_ref, fresh_ref, out, fresh):
    out[...] = out_ref[...]
    fresh[...] = fresh_ref[...]


def body(
    seq,
    tensor,
    hidden,
    pre_gain,
    w_query,
    w_key,
    w_value,
    w_out,
    post_gain,
    cache_pool,
    prompt_cache,
    task_ids,
    cache_lengths,
    block_table,
):
    rows, width = hidden.shape
    cols = post_gain.shape[0]
    heads = w_query.shape[1] // HD
    pages = cache_pool.shape[0]
    lines = rows * cols // HD
    pieces = 6
    half = HD // 2
    freq = np.float32(10000.0) ** (-np.arange(half, dtype=np.float64) / half)
    freq = jnp.asarray(np.concatenate([freq, freq])[None].astype(np.float32))
    args = (
        hidden,
        pre_gain,
        w_query,
        w_key,
        w_value,
        w_out,
        post_gain,
        cache_pool,
        prompt_cache,
        task_ids.reshape(1, -1),
        cache_lengths.reshape(1, -1),
        block_table.T,
        freq,
    )
    wide = (heads + 1) * HD
    dma = pltpu.SemaphoreType.DMA
    outs = pl.pallas_call(
        functools.partial(layer, seq=seq, tensor=tensor, pieces=pieces),
        out_shape=(
            pltpu.VMEM((rows, cols), BF16),
            pltpu.VMEM((rows, 2, HD), BF16),
        ),
        in_specs=[pl.BlockSpec(memory_space=pltpu.HBM)] * len(args),
        out_specs=[pl.BlockSpec(memory_space=pltpu.VMEM)] * 2,
        scratch_shapes=[pltpu.VMEM(a.shape, a.dtype) for a in args]
        + [
            pltpu.VMEM((pages, wide), F32),
            pltpu.VMEM((seq, heads * rows, HD), F32),
            pltpu.VMEM((seq, heads * rows, HD), F32),
            pltpu.VMEM((seq, rows, HD), jnp.int32),
            pltpu.VMEM((seq, rows, heads * HD), BF16),
            pltpu.VMEM((seq, heads * rows + 8, HD), BF16),
            pltpu.VMEM((seq, heads * rows + 8, HD), BF16),
            pltpu.VMEM((tensor, lines, HD), BF16),
            pltpu.VMEM((tensor, lines, HD), BF16),
            pltpu.VMEM((tensor, 1, HD), F32),
            pltpu.SemaphoreType.REGULAR((tensor,)),
            dma((10,)),
            dma((pieces,)),
            dma,
            dma((seq,)),
        ]
        + [dma] * 6,
        compiler_params=pltpu.CompilerParams(
            collective_id=0, has_side_effects=True, vmem_limit_bytes=60 * 1024 * 1024
        ),
        name="layer",
    )(*args)
    return pl.pallas_call(
        hand_out,
        out_shape=tuple(jax.ShapeDtypeStruct(a.shape, a.dtype) for a in outs),
        in_specs=[pl.BlockSpec(memory_space=pltpu.VMEM)] * 2,
        out_specs=[pl.BlockSpec(memory_space=pltpu.VMEM)] * 2,
        name="hand_out",
    )(*(pltpu.with_memory_space_constraint(a, pltpu.VMEM) for a in outs))


def solution(mesh):
    seq = mesh.shape["seq"]
    tensor = mesh.shape["tensor"]
    return jax.shard_map(
        functools.partial(body, seq, tensor),
        mesh=mesh,
        in_specs=(
            P(("groups", "seq"), None),
            P(),
            P(None, "tensor"),
            P(None, "tensor"),
            P(None, "tensor"),
            P("tensor", None),
            P("tensor"),
            P(("groups", "seq"), None, None, "tensor"),
            P("seq", None, None, "tensor"),
            P("groups"),
            P("groups"),
            P("groups", None),
        ),
        out_specs=(P(("groups", "seq"), "tensor"), P(("groups", "seq"), None, "tensor")),
        check_vma=False,
    )
```
